512 devices in a mesh: row: 16 (over y_lo, z), col: 8 (over x, core), dp: 4 (over y_hi).
Axes of the slice: x: 4, y: 8 (y_hi: 4, y_lo: 2; y = y_hi * 2 + y_lo), z: 8, core: 2. Of those that a mesh axis runs over, the one named last changes fastest.
Arguments:
- tokens: bfloat16 [1536, 6144], P('dp', 'row'), parts along dimension 0, may hold values from -120 to 120
- norm_gain: float32 [6144], P('row'), may hold values from 0.25 to 1.75
- qkv_weight: bfloat16 [6144, 3, 3072], P('row', None, 'col'), may hold values from -2.5 to 2.5
- out_weight: bfloat16 [3072, 6144], P('col', 'row'), may hold values from -0.109375 to 0.109375
Outputs:
- projected: bfloat16 [1536, 6144], P('dp', 'row'), parts along dimension 0
The draws below stay inside these ranges and needn't reach their ends.
There are 4 independent parts, one for each index of `dp`. The reference program is written for one: setup_inputs(seed, part) draws one part's arguments, and reference() takes and returns one part's arrays. A program takes and returns all parts, laid end to end along the dimension named above; an argument that names none is the same for every part. Nothing has to cross between parts.
All inputs are finite; a program needn't handle non-finite values.
Results may differ from the reference program's by a relative error of at most 0.025.
Values may be sent and summed in bfloat16 or wider, within the bound.
A program may use at most 64 MiB of HBM per device.

```python
import math
import jax
import jax.numpy as jnp
from jax import lax

D = 6144
H = 24
K = 128
SEQ = 384
N_ROW = 16


def draw_tokens(key, part):
    subkeys = jax.random.split(key, 4)
    position = jnp.arange(D, dtype=jnp.float32) / D
    texture = jnp.exp(jax.random.uniform(subkeys[0], (1, D), jnp.float32, jnp.log(0.7), jnp.log(1.4)))
    row_scale = jnp.exp(jax.random.uniform(subkeys[1], (SEQ, 1), jnp.float32, jnp.log(0.5), jnp.log(2.0)))
    offset = jnp.clip(jax.random.normal(subkeys[2], (SEQ, 1), jnp.float32), -3.0, 3.0)
    feature_ramp = 10.0 ** (position - 0.5)
    jitter = jnp.clip(jax.random.normal(subkeys[3], (SEQ, D), jnp.float32), -4.0, 4.0)
    values = row_scale * feature_ramp * (offset + jitter * texture)
    return jnp.clip(values, -120.0, 120.0).astype(jnp.bfloat16)


def draw_qkv_weight(key, part):
    subkeys = jax.random.split(key, 1)
    weights = jnp.clip(jax.random.normal(subkeys[0], (D, 3, H * K), jnp.float32), -6.0, 6.0) / math.sqrt(D)
    return jnp.clip(weights, -2.5, 2.5).astype(jnp.bfloat16)


def block_scale(own_key, dims, cuts, low, top_value):
    level = 1.0
    for axis_at, blocks in cuts:
        heights = jax.random.uniform(jax.random.fold_in(jax.random.fold_in(own_key, 6), axis_at), (blocks,), jnp.float32, low / len(cuts), top_value / len(cuts))
        level = level * jnp.repeat(jnp.exp(heights), dims[axis_at] // blocks).reshape((-1,) + (1,) * (len(dims) - 1 - axis_at))
    return level


def bell_draw(stream_key, dims, deviation, reach, shards=(), kind=jnp.bfloat16):
    level = block_scale(stream_key, dims, shards, -0.22, 0.18) if shards else 1.0
    entries = jax.random.normal(stream_key, dims, jnp.float32) * deviation * level
    return jnp.minimum(jnp.maximum(entries, -reach), reach).astype(kind)


def setup_inputs(seed: int = 0, part: int = 0) -> dict:
    key_of = jax.random.split(jax.random.key(seed), 5)
    part_splits = jax.random.split(jax.random.fold_in(key_of[4], part), 5)
    return {
        "tokens": draw_tokens(jax.random.fold_in(jax.random.fold_in(key_of[4], part), 71), part),
        "norm_gain": jnp.clip(1.0 + 0.15 * jax.random.normal(key_of[1], (D,), jnp.float32), 0.25, 1.75),
        "qkv_weight": draw_qkv_weight(jax.random.fold_in(key_of[4], 71), part),
        "out_weight": bell_draw(key_of[3], (H * K, D), (H * K) ** -0.5, 0.109375, ((0, 8), (1, 16))),
    }


EPSILON = 1e-05

def normalize(tokens, norm_gain):
    values = tokens.astype(jnp.float32)
    average = lax.optimization_barrier(jnp.mean(values, axis=1, keepdims=True))
    centered = values - average
    variance = lax.optimization_barrier(jnp.mean(centered * centered, axis=1, keepdims=True))
    return (centered * lax.rsqrt(variance + EPSILON) * norm_gain).astype(jnp.bfloat16)

def project(normed, qkv_weight):
    block_width = D // N_ROW
    flattened = qkv_weight.reshape(D, 3 * H * K)
    totals = jnp.zeros((SEQ, 3 * H * K), jnp.float32)
    for row_block in range(N_ROW):
        first_feature = row_block * block_width
        partial_value = jnp.dot(normed[:, first_feature:first_feature + block_width], flattened[first_feature:first_feature + block_width], preferred_element_type=jnp.float32)
        rounded = lax.optimization_barrier(partial_value.astype(jnp.bfloat16))
        totals = totals + rounded.astype(jnp.float32)
    return totals.astype(jnp.bfloat16).reshape(SEQ, 3, H, K)

def attend_head(operands):
    query_part, key_part, value_part = operands
    scores = jnp.dot(query_part, key_part.T, preferred_element_type=jnp.float32) * (1.0 / math.sqrt(K))
    largest = lax.optimization_barrier(jnp.max(scores, axis=1, keepdims=True))
    exponent = jnp.exp(scores - largest)
    softmax_weights = (exponent / lax.optimization_barrier(jnp.sum(exponent, axis=1, keepdims=True))).astype(jnp.bfloat16)
    return jnp.dot(softmax_weights, value_part, preferred_element_type=jnp.float32).astype(jnp.bfloat16)

def reference(tokens, norm_gain, qkv_weight, out_weight):
    normed = normalize(tokens, norm_gain)
    stacked = jnp.transpose(project(normed, qkv_weight), (1, 2, 0, 3))
    attended = lax.map(attend_head, (stacked[0], stacked[1], stacked[2]))
    attended = jnp.transpose(attended, (1, 0, 2)).reshape(SEQ, H * K)
    return jnp.dot(attended, out_weight, preferred_element_type=jnp.float32).astype(jnp.bfloat16)
```

```python
import math

import jax
import jax.numpy as jnp
from jax import lax
from jax.experimental import pallas as pl
from jax.experimental.pallas import tpu as pltpu
from jax.sharding import PartitionSpec as P

K = 128
EPSILON = 1e-05
F32 = jnp.float32
BF16 = jnp.bfloat16
T = 384
HALF = 192
BLOCK = 48
ZS = 8
COLS = 8
FEATURES = 6144
ORDER = (1, 2, 0)
MESH = pl.DeviceIdType.MESH


def owner_z(owner):
    return owner + owner // 2


def kernel(
    x_hbm, gain_ref, w_hbm, wo_hbm, o_ref,
    x_v, w_v, wo_v, lhs, aux_own, aux_all, part, y_buf, z_buf, z_in, acc, qkv, tall, att, p_buf, p_in,
    load_sem, aux_sems, auxz_send, auxz_recv, y_send, y_recv, z_send, z_recv,
    kv_send, kv_recv, at_send, at_recv, ay_send, ay_recv, rs_send, rs_recv, ag_send, ag_recv,
):
    row = lax.axis_index("row")
    col = lax.axis_index("col")
    y = row // ZS
    z = row % ZS
    active = y == col % 2
    partner = {"row": (1 - y) * ZS + z}
    is_owner = jnp.logical_and(active, z % 3 != 2)
    mine = z - (z + 1) // 3
    head = mine // 2
    half = mine % 2

    def at_z(other):
        return {"row": y * ZS + other}

    def remote(src, dst, send, recv, device):
        return pltpu.make_async_remote_copy(
            src_ref=src, dst_ref=dst, send_sem=send, recv_sem=recv, device_id=device, device_id_type=MESH
        )

    x_load = pltpu.make_async_copy(x_hbm, x_v, load_sem.at[0])
    x_load.start()
    w_loads = [pltpu.make_async_copy(w_hbm.at[j], w_v.at[j], load_sem.at[1 + j]) for j in range(3)]
    for j in ORDER:
        w_loads[j].start()
    wo_load = pltpu.make_async_copy(wo_hbm, wo_v, load_sem.at[4])
    wo_load.start()

    barrier = pltpu.get_barrier_semaphore()
    pl.semaphore_signal(barrier, inc=1, device_id=partner, device_id_type=MESH)
    for d in range(1, ZS):
        pl.semaphore_signal(barrier, inc=1, device_id=at_z((z + d) % ZS), device_id_type=MESH)
    for d in range(1, COLS):
        pl.semaphore_signal(barrier, inc=1, device_id={"col": (col + d) % COLS}, device_id_type=MESH)

    x_load.wait()
    values = x_v[...].astype(F32)
    mean = jnp.sum(values, axis=1, keepdims=True) * (1.0 / T)
    centered = values - mean
    squares = jnp.sum(centered * centered, axis=1, keepdims=True)
    gain = gain_ref[...].reshape(1, T)
    lhs[0:T, :] = (centered * gain).astype(BF16)
    high = gain.astype(BF16).astype(F32)
    rows = lax.broadcasted_iota(jnp.int32, (16, T), 0)
    lhs[T : T + 16, :] = jnp.where(rows == 0, high, jnp.where(rows == 1, gain - high, 0.0)).astype(BF16)
    lanes = lax.broadcasted_iota(jnp.int32, (T, 128), 1)
    turned = jnp.where(lanes == 0, mean, jnp.where(lanes == 1, squares, 0.0)).T
    aux_own[0:8, :] = turned[0:8, :]

    y_copies = [
        remote(y_buf.at[u], y_buf.at[u], y_send.at[u], y_recv.at[u], partner) for u in range(9)
    ]
    aux_copy = remote(aux_own, aux_all.at[z, 1], aux_sems.at[0], aux_sems.at[1], partner)

    for step, j in enumerate(ORDER):
        w_loads[j].wait()
        product = jnp.dot(lhs[...], w_v[j], preferred_element_type=F32)
        aux_own[2 + j : 3 + j, :] = product[T : T + 1, :] + product[T + 1 : T + 2, :]

        @pl.when(active)
        def _():
            for h in range(3):
                part[3 * j + h] = product[0:T, h * K : (h + 1) * K]

        @pl.when(jnp.logical_not(active))
        def _():
            for h in range(3):
                y_buf[3 * j + h] = product[0:T, h * K : (h + 1) * K].astype(BF16)

        if step == 0:
            pl.semaphore_wait(barrier, 1 + (ZS - 1) + (COLS - 1))

        @pl.when(jnp.logical_not(active))
        def _():
            for h in range(3):
                y_copies[3 * j + h].start()

    @pl.when(jnp.logical_not(active))
    def _():
        aux_copy.start()

    def z_copy(u, o):
        return remote(
            z_buf.at[u, o % 2], z_in.at[z, u // 3], z_send.at[u, o % 2], z_recv.at[z, u // 3], at_z(owner_z(o))
        )

    def aux_z_copy(o):
        return remote(aux_all.at[z], aux_all.at[z], auxz_send.at[o], auxz_recv.at[z], at_z(owner_z(o)))

    @pl.when(active)
    def _():
        aux_all[z, 0] = aux_own[...]
        aux_copy.wait_recv()
        for o in range(6):
            @pl.when(z != owner_z(o))
            def _(o=o):
                aux_z_copy(o).start()

        for j in ORDER:
            for h in range(3):
                u = 3 * j + h
                y_copies[u].wait_recv()
                for s in range(2):
                    o = 2 * h + s
                    tokens = slice(s * HALF, (s + 1) * HALF)
                    total = part[u, tokens, :] + y_buf[u, tokens, :].astype(F32)

                    @pl.when(z != owner_z(o))
                    def _(o=o, u=u, s=s, total=total):
                        z_buf[u, s] = total.astype(BF16)
                        z_copy(u, o).start()

                    @pl.when(z == owner_z(o))
                    def _(j=j, total=total):
                        acc[j] = total

    kv_copy = remote(
        qkv.at[pl.ds(1, 2), half], qkv.at[pl.ds(1, 2), half], kv_send.at[0], kv_recv.at[0], at_z(z + 1 - 2 * half)
    )

    def at_copy(o, d):
        return remote(att.at[o], att.at[o], at_send.at[d - 1], at_recv.at[o], at_z((z + d) % ZS))

    def ay_copy(o):
        return remote(att.at[o], att.at[o], ay_send.at[o], ay_recv.at[o], partner)

    @pl.when(is_owner)
    def _():
        for d in range(1, ZS):
            other = (z + d) % ZS
            remote(
                aux_all.at[other], aux_all.at[other], auxz_send.at[0], auxz_recv.at[other], at_z(other)
            ).wait_recv()
        flat = aux_all[...].reshape(2 * ZS, 8, T)
        means = flat[:, 0, :]
        average = jnp.sum(means, axis=0, keepdims=True) * (1.0 / 16)
        offsets = means - average
        spread = jnp.sum(flat[:, 1, :] + T * (offsets * offsets), axis=0, keepdims=True) * (1.0 / FEATURES)
        scale = lax.rsqrt(spread + EPSILON)
        stacked = jnp.concatenate([offsets, jnp.broadcast_to(scale, (112, T))], axis=0)
        tall[...] = stacked.T
        tall_half = tall[pl.ds(pl.multiple_of(half * HALF, HALF), HALF), :]
        scale_col = tall_half[:, 16:17]
        offset_cols = tall_half[:, 0:16]
        lane0 = pl.multiple_of(head * K, K)

        for j in ORDER:
            weights_sum = aux_all[:, :, 2 + j, pl.ds(lane0, K)].reshape(2 * ZS, K)
            total = acc[j] + jnp.dot(
                offset_cols, weights_sum, preferred_element_type=F32, precision=lax.Precision.HIGHEST
            )
            for d in range(1, ZS):
                other = (z + d) % ZS
                remote(
                    z_in.at[other, j], z_in.at[other, j], z_send.at[0, 0], z_recv.at[other, j], at_z(other)
                ).wait_recv()
                total = total + z_in[other, j].astype(F32)
            qkv[j, half] = (total * scale_col).astype(BF16)
            if j == 2:
                kv_copy.start()

        kv_copy.wait_recv()
        queries = qkv[0, half]
        keys = qkv[1].reshape(T, K)
        scores = lax.dot_general(
            queries, keys, (((1,), (1,)), ((), ())), preferred_element_type=F32
        ) * (1.0 / math.sqrt(K))
        exponent = jnp.exp(scores - jnp.max(scores, axis=1, keepdims=True))
        weights = (exponent / jnp.sum(exponent, axis=1, keepdims=True)).astype(BF16)
        mixed = jnp.dot(weights, qkv[2].reshape(T, K), preferred_element_type=F32)
        att[mine] = mixed.astype(BF16)
        for d in range(1, ZS):
            at_copy(mine, d).start()

    @pl.when(active)
    def _():
        for o in range(6):
            @pl.when(z != owner_z(o))
            def _(o=o):
                at_copy(o, 1).wait_recv()
            ay_copy(o).start()

    wo_load.wait()

    @pl.when(jnp.logical_not(active))
    def _():
        for o in range(6):
            ay_copy(o).wait_recv()

    for s in range(2):
        attended = jnp.concatenate([att[2 * h + s] for h in range(3)], axis=1)
        product = jnp.dot(attended, wo_v[...], preferred_element_type=F32).astype(BF16)
        for b in range(4):
            p_buf[4 * s + b] = product[b * BLOCK : (b + 1) * BLOCK, :]

    def rs_copy(d):
        other = (col + d) % COLS
        return remote(p_buf.at[other], p_in.at[col], rs_send.at[d - 1], rs_recv.at[col], {"col": other})

    def rs_arrival(d):
        other = (col + d) % COLS
        return remote(p_buf.at[col], p_in.at[other], rs_send.at[d - 1], rs_recv.at[other], {"col": other})

    my_rows = o_ref.at[pl.ds(pl.multiple_of(col * BLOCK, BLOCK), BLOCK), :]

    def ag_copy(d):
        other = (col + d) % COLS
        return remote(my_rows, my_rows, ag_send.at[d - 1], ag_recv.at[col], {"col": other})

    def ag_arrival(d):
        other = (col + d) % COLS
        rows_there = o_ref.at[pl.ds(pl.multiple_of(other * BLOCK, BLOCK), BLOCK), :]
        return remote(rows_there, rows_there, ag_send.at[d - 1], ag_recv.at[other], {"col": other})

    for d in range(1, COLS):
        rs_copy(d).start()
    total = p_buf[col].astype(F32)
    for d in range(1, COLS):
        rs_arrival(d).wait_recv()
        total = total + p_in[(col + d) % COLS].astype(F32)
    my_rows[...] = total.astype(BF16)
    for d in range(1, COLS):
        ag_copy(d).start()

    @pl.when(jnp.logical_not(active))
    def _():
        aux_copy.wait_send()
        for u in range(9):
            y_copies[u].wait_send()

    @pl.when(active)
    def _():
        for o in range(6):
            ay_copy(o).wait_send()

            @pl.when(z != owner_z(o))
            def _(o=o):
                aux_z_copy(o).wait_send()
                for j in range(3):
                    z_copy(3 * j + o // 2, o).wait_send()

    @pl.when(is_owner)
    def _():
        kv_copy.wait_send()
        for d in range(1, ZS):
            at_copy(mine, d).wait_send()

    for d in range(1, COLS):
        rs_copy(d).wait_send()
        ag_arrival(d).wait_recv()
    for d in range(1, COLS):
        ag_copy(d).wait_send()


def shards(tokens, norm_gain, qkv_weight, out_weight):
    dma = pltpu.SemaphoreType.DMA
    return pl.pallas_call(
        kernel,
        out_shape=jax.ShapeDtypeStruct((T, T), BF16),
        in_specs=[
            pl.BlockSpec(memory_space=pl.ANY),
            pl.BlockSpec(memory_space=pltpu.VMEM),
            pl.BlockSpec(memory_space=pl.ANY),
            pl.BlockSpec(memory_space=pl.ANY),
        ],
        out_specs=pl.BlockSpec(memory_space=pltpu.VMEM),
        scratch_shapes=[
            pltpu.VMEM((T, T), BF16),
            pltpu.VMEM((3, T, T), BF16),
            pltpu.VMEM((T, T), BF16),
            pltpu.VMEM((T + 16, T), BF16),
            pltpu.VMEM((8, T), F32),
            pltpu.VMEM((ZS, 2, 8, T), F32),
            pltpu.VMEM((9, T, K), F32),
            pltpu.VMEM((9, T, K), BF16),
            pltpu.VMEM((9, 2, HALF, K), BF16),
            pltpu.VMEM((ZS, 3, HALF, K), BF16),
            pltpu.VMEM((3, HALF, K), F32),
            pltpu.VMEM((3, 2, HALF, K), BF16),
            pltpu.VMEM((T, 128), F32),
            pltpu.VMEM((6, HALF, K), BF16),
            pltpu.VMEM((COLS, BLOCK, T), BF16),
            pltpu.VMEM((COLS, BLOCK, T), BF16),
            dma((5,)),
            dma((2,)),
            dma((6,)),
            dma((ZS,)),
            dma((9,)),
            dma((9,)),
            dma((9, 2)),
            dma((ZS, 3)),
            dma((1,)),
            dma((1,)),
            dma((ZS - 1,)),
            dma((6,)),
            dma((6,)),
            dma((6,)),
            dma((COLS - 1,)),
            dma((COLS,)),
            dma((COLS - 1,)),
            dma((COLS,)),
        ],
        compiler_params=pltpu.CompilerParams(collective_id=0, has_side_effects=True),
        name="sublayer",
    )(tokens, norm_gain, jnp.transpose(qkv_weight, (1, 0, 2)), out_weight)


def solution(mesh):
    in_specs = (P("dp", "row"), P("row"), P("row", None, "col"), P("col", "row"))
    out_specs = P("dp", "row")
    return jax.shard_map(shards, mesh=mesh, in_specs=in_specs, out_specs=out_specs, check_vma=False)
```

```python
import math

import jax
import jax.numpy as jnp
from jax import lax
from jax.experimental import pallas as pl
from jax.experimental.pallas import tpu as pltpu
from jax.sharding import PartitionSpec as P

K = 128
EPSILON = 1e-05
F32 = jnp.float32
BF16 = jnp.bfloat16
T = 384
HALF = 192
BLOCK = 48
ZS = 8
COLS = 8
FEATURES = 6144
ORDER = (1, 2, 0)
MESH = pl.DeviceIdType.MESH


def owner_z(owner):
    return owner + owner // 3


def kernel(
    x_hbm, gain_hbm, w_hbm, wo_hbm, o_ref,
    x_v, gain_v, w_v, wo_v, lhs, aux_own, aux_all, part, y_buf, z_buf, z_in, acc, qkv, att, p_buf, p_in,
    load_sem, aux_sems, auxz_send, auxz_recv, y_send, y_recv, z_send, z_recv,
    kv_send, kv_recv, at_send, at_recv, ay_send, ay_recv, rs_send, rs_recv, ag_send, ag_recv,
):
    row = lax.axis_index("row")
    col = lax.axis_index("col")
    y = row // ZS
    z = row % ZS
    active = y == col % 2
    partner = {"row": (1 - y) * ZS + z}
    is_owner = jnp.logical_and(active, z % 4 != 3)
    mine = z - z // 4
    head = mine // 2
    half = mine % 2

    def at_z(other):
        return {"row": y * ZS + other}

    def remote(src, dst, send, recv, device):
        return pltpu.make_async_remote_copy(
            src_ref=src, dst_ref=dst, send_sem=send, recv_sem=recv, device_id=device, device_id_type=MESH
        )

    x_load = pltpu.make_async_copy(x_hbm, x_v, load_sem.at[0])
    x_load.start()
    w_loads = [pltpu.make_async_copy(w_hbm.at[j], w_v.at[j], load_sem.at[1 + j]) for j in range(3)]
    for j in ORDER:
        w_loads[j].start()
    gain_load = pltpu.make_async_copy(gain_hbm, gain_v, load_sem.at[5])
    gain_load.start()
    wo_load = pltpu.make_async_copy(wo_hbm, wo_v, load_sem.at[4])
    wo_load.start()

    barrier = pltpu.get_barrier_semaphore()
    pl.semaphore_signal(barrier, inc=1, device_id=partner, device_id_type=MESH)
    for d in range(1, ZS):
        pl.semaphore_signal(barrier, inc=1, device_id=at_z((z + d) % ZS), device_id_type=MESH)
    for d in range(1, COLS):
        pl.semaphore_signal(barrier, inc=1, device_id={"col": (col + d) % COLS}, device_id_type=MESH)

    x_load.wait()
    values = x_v[...].astype(F32)
    mean = jnp.sum(values, axis=1, keepdims=True) * (1.0 / T)
    centered = values - mean
    squares = jnp.sum(centered * centered, axis=1, keepdims=True)
    gain_load.wait()
    gain = gain_v[...].reshape(1, T)
    lhs[0:T, :] = (centered * gain).astype(BF16)
    high = gain.astype(BF16).astype(F32)
    rows = lax.broadcasted_iota(jnp.int32, (16, T), 0)
    lhs[T : T + 16, :] = jnp.where(rows == 0, high, jnp.where(rows == 1, gain - high, 0.0)).astype(BF16)
    lanes = lax.broadcasted_iota(jnp.int32, (T, 128), 1)
    turned = jnp.where(lanes == 0, mean, jnp.where(lanes == 1, squares, 0.0)).T
    early = turned[0:8, :]
    late = pltpu.roll(early, T - HALF, 1)
    for o in range(6):
        source = early if o % 2 == 0 else late
        for r in range(2):
            aux_own[0, o, 3 + 2 * r : 4 + 2 * r, :] = source[r : r + 1, 0:K]
            aux_own[0, o, 4 + 2 * r : 5 + 2 * r, :] = source[r : r + 1, K : 2 * K]

    y_copies = [
        remote(y_buf.at[u], y_buf.at[u], y_send.at[u], y_recv.at[u], partner) for u in range(9)
    ]
    aux_copy = remote(aux_own.at[0], aux_own.at[1], aux_sems.at[0], aux_sems.at[1], partner)

    for step, j in enumerate(ORDER):
        w_loads[j].wait()
        product = jnp.dot(lhs[...], w_v[j], preferred_element_type=F32)
        weights_sum = product[T : T + 1, :] + product[T + 1 : T + 2, :]
        for o in range(6):
            aux_own[0, o, j : j + 1, :] = weights_sum[:, (o // 2) * K : (o // 2 + 1) * K]

        @pl.when(active)
        def _():
            for h in range(3):
                part[3 * j + h] = product[0:T, h * K : (h + 1) * K]

        @pl.when(jnp.logical_not(active))
        def _():
            for h in range(3):
                y_buf[3 * j + h] = product[0:T, h * K : (h + 1) * K].astype(BF16)

        if step == 0:
            pl.semaphore_wait(barrier, 1 + (ZS - 1) + (COLS - 1))

        @pl.when(jnp.logical_not(active))
        def _(step=step):
            if step == 0:
                for h in range(3):
                    y_copies[3 * ORDER[0] + h].start()
            if step == 2:
                aux_copy.start()
                for later in ORDER[1:]:
                    for h in range(3):
                        y_copies[3 * later + h].start()

    def z_copy(u, o):
        return remote(
            z_buf.at[u, o % 2], z_in.at[z, u // 3], z_send.at[u, o % 2], z_recv.at[z, u // 3], at_z(owner_z(o))
        )

    def aux_z_copy(o):
        return remote(aux_own.at[:, o], aux_all.at[z], auxz_send.at[o], auxz_recv.at[z], at_z(owner_z(o)))

    @pl.when(active)
    def _():
        for j in ORDER:
            for h in range(3):
                u = 3 * j + h
                y_copies[u].wait_recv()
                for s in range(2):
                    o = 2 * h + s
                    tokens = slice(s * HALF, (s + 1) * HALF)
                    total = part[u, tokens, :] + y_buf[u, tokens, :].astype(F32)

                    @pl.when(z != owner_z(o))
                    def _(o=o, u=u, s=s, total=total):
                        z_buf[u, s] = total.astype(BF16)
                        z_copy(u, o).start()

                    @pl.when(z == owner_z(o))
                    def _(j=j, total=total):
                        acc[j] = total

            if j == ORDER[0]:
                aux_copy.wait_recv()
                for o in range(6):
                    @pl.when(z != owner_z(o))
                    def _(o=o):
                        aux_z_copy(o).start()

                    @pl.when(z == owner_z(o))
                    def _(o=o):
                        aux_all[z] = aux_own[:, o]

    kv_copy = remote(
        qkv.at[pl.ds(1, 2), half], qkv.at[pl.ds(1, 2), half], kv_send.at[0], kv_recv.at[0], at_z(owner_z(mine + 1 - 2 * half))
    )

    def at_copy(o, d):
        return remote(att.at[o], att.at[o], at_send.at[d - 1], at_recv.at[o], at_z((z + d) % ZS))

    def ay_copy(o):
        return remote(att.at[o], att.at[o], ay_send.at[o], ay_recv.at[o], partner)

    @pl.when(is_owner)
    def _():
        for d in range(1, ZS):
            other = (z + d) % ZS
            remote(
              aux_all.at[other], aux_all.at[other], auxz_send.at[0], auxz_recv.at[other], at_z(other)
            ).wait_recv()
        def gathered(r):
            return aux_all[:, :, r, :].reshape(2 * ZS, K)

        means = jnp.concatenate([gathered(3), gathered(4)], axis=1)
        average = jnp.sum(means, axis=0, keepdims=True) * (1.0 / 16)
        offsets = means - average
        sums = jnp.concatenate([gathered(5), gathered(6)], axis=1)
        spread = jnp.sum(sums + T * (offsets * offsets), axis=0, keepdims=True) * (1.0 / FEATURES)
        scale = lax.rsqrt(spread + EPSILON)
        tall = jnp.concatenate([offsets, jnp.broadcast_to(scale, (112, 2 * K))], axis=0).T
        scale_col = tall[0:HALF, 16:17]
        offset_cols = tall[0:HALF, 0:16]

        for j in ORDER:
            total = acc[j] + jnp.dot(
                offset_cols, gathered(j), preferred_element_type=F32, precision=lax.Precision.HIGHEST
            )
            for d in range(1, ZS):
                other = (z + d) % ZS
                remote(
                  z_in.at[other, j], z_in.at[other, j], z_send.at[0, 0], z_recv.at[other, j], at_z(other)
                ).wait_recv()
                total = total + z_in[other, j].astype(F32)
            qkv[j, half] = (total * scale_col).astype(BF16)
            if j == 2:
                kv_copy.start()

        kv_copy.wait_recv()
        queries = qkv[0, half]
        keys = qkv[1].reshape(T, K)
        scores = lax.dot_general(
            queries, keys, (((1,), (1,)), ((), ())), preferred_element_type=F32
        ) * (1.0 / math.sqrt(K))
        exponent = jnp.exp(scores - jnp.max(scores, axis=1, keepdims=True))
        weights = (exponent / jnp.sum(exponent, axis=1, keepdims=True)).astype(BF16)
        mixed = jnp.dot(weights, qkv[2].reshape(T, K), preferred_element_type=F32)
        att[mine] = mixed.astype(BF16)
        for d in range(1, ZS):
            at_copy(mine, d).start()

    @pl.when(active)
    def _():
        for o in range(6):
            @pl.when(z != owner_z(o))
            def _(o=o):
                at_copy(o, 1).wait_recv()
            ay_copy(o).start()

    wo_load.wait()

    @pl.when(jnp.logical_not(active))
    def _():
        for o in range(6):
            ay_copy(o).wait_recv()

    for s in range(2):
        attended = jnp.concatenate([att[2 * h + s] for h in range(3)], axis=1)
        product = jnp.dot(attended, wo_v[...], preferred_element_type=F32).astype(BF16)
        for b in range(4):
            p_buf[4 * s + b] = product[b * BLOCK : (b + 1) * BLOCK, :]

    def rs_copy(d):
        other = (col + d) % COLS
        return remote(p_buf.at[other], p_in.at[col], rs_send.at[d - 1], rs_recv.at[col], {"col": other})

    def rs_arrival(d):
        other = (col + d) % COLS
        return remote(p_buf.at[col], p_in.at[other], rs_send.at[d - 1], rs_recv.at[other], {"col": other})

    my_rows = o_ref.at[pl.ds(pl.multiple_of(col * BLOCK, BLOCK), BLOCK), :]

    def ag_copy(d):
        other = (col + d) % COLS
        return remote(my_rows, my_rows, ag_send.at[d - 1], ag_recv.at[col], {"col": other})

    def ag_arrival(d):
        other = (col + d) % COLS
        rows_there = o_ref.at[pl.ds(pl.multiple_of(other * BLOCK, BLOCK), BLOCK), :]
        return remote(rows_there, rows_there, ag_send.at[d - 1], ag_recv.at[other], {"col": other})

    for d in range(1, COLS):
        rs_copy(d).start()
    total = p_buf[col].astype(F32)
    for d in range(1, COLS):
        rs_arrival(d).wait_recv()
        total = total + p_in[(col + d) % COLS].astype(F32)
    my_rows[...] = total.astype(BF16)
    for d in range(1, COLS):
        ag_copy(d).start()

    @pl.when(jnp.logical_not(active))
    def _():
        aux_copy.wait_send()
        for u in range(9):
            y_copies[u].wait_send()

    @pl.when(active)
    def _():
        for o in range(6):
            ay_copy(o).wait_send()

            @pl.when(z != owner_z(o))
            def _(o=o):
                aux_z_copy(o).wait_send()
                for j in range(3):
                    z_copy(3 * j + o // 2, o).wait_send()

    @pl.when(is_owner)
    def _():
        kv_copy.wait_send()
        for d in range(1, ZS):
            at_copy(mine, d).wait_send()

    for d in range(1, COLS):
        rs_copy(d).wait_send()
        ag_arrival(d).wait_recv()
    for d in range(1, COLS):
        ag_copy(d).wait_send()


def shards(tokens, norm_gain, qkv_weight, out_weight):
    dma = pltpu.SemaphoreType.DMA
    return pl.pallas_call(
        kernel,
        out_shape=pltpu.VMEM((T, T), BF16),
        in_specs=[
            pl.BlockSpec(memory_space=pl.ANY),
            pl.BlockSpec(memory_space=pl.ANY),
            pl.BlockSpec(memory_space=pl.ANY),
            pl.BlockSpec(memory_space=pl.ANY),
        ],
        out_specs=pl.BlockSpec(memory_space=pltpu.VMEM),
        scratch_shapes=[
            pltpu.VMEM((T, T), BF16),
            pltpu.VMEM((T,), F32),
            pltpu.VMEM((3, T, T), BF16),
            pltpu.VMEM((T, T), BF16),
            pltpu.VMEM((T + 16, T), BF16),
            pltpu.VMEM((2, 6, 8, K), F32),
            pltpu.VMEM((ZS, 2, 8, K), F32),
            pltpu.VMEM((9, T, K), F32),
            pltpu.VMEM((9, T, K), BF16),
            pltpu.VMEM((9, 2, HALF, K), BF16),
            pltpu.VMEM((ZS, 3, HALF, K), BF16),
            pltpu.VMEM((3, HALF, K), F32),
            pltpu.VMEM((3, 2, HALF, K), BF16),
            pltpu.VMEM((6, HALF, K), BF16),
            pltpu.VMEM((COLS, BLOCK, T), BF16),
            pltpu.VMEM((COLS, BLOCK, T), BF16),
            dma((6,)),
            dma((2,)),
            dma((6,)),
            dma((ZS,)),
            dma((9,)),
            dma((9,)),
            dma((9, 2)),
            dma((ZS, 3)),
            dma((1,)),
            dma((1,)),
            dma((ZS - 1,)),
            dma((6,)),
            dma((6,)),
            dma((6,)),
            dma((COLS - 1,)),
            dma((COLS,)),
            dma((COLS - 1,)),
            dma((COLS,)),
        ],
        compiler_params=pltpu.CompilerParams(collective_id=0, has_side_effects=True),
        name="sublayer",
    )(tokens, norm_gain, jnp.transpose(qkv_weight, (1, 0, 2)), out_weight)


def solution(mesh):
    in_specs = (P("dp", "row"), P("row"), P("row", None, "col"), P("col", "row"))
    out_specs = P("dp", "row")
    return jax.shard_map(shards, mesh=mesh, in_specs=in_specs, out_specs=out_specs, check_vma=False)
```

```python
import math

import jax
import jax.numpy as jnp
from jax import lax
from jax.experimental import pallas as pl
from jax.experimental.pallas import tpu as pltpu
from jax.sharding import PartitionSpec as P

K = 128
EPSILON = 1e-05
F32 = jnp.float32
BF16 = jnp.bfloat16
T = 384
HALF = 192
BLOCK = 48
ZS = 8
COLS = 8
FEATURES = 6144
ORDER = (1, 2, 0)
EARLY = 2
MESH = pl.DeviceIdType.MESH


def owner_z(owner):
    return owner + owner // 3


def kernel(
    x_hbm, gain_hbm, w_hbm, wo_hbm, o_ref,
    x_v, gain_v, w_v, wo_v, lhs, aux_own, aux_all, part, y_buf, z_buf, z_in, tie_in, acc, qkv, att, p_buf, p_in,
    load_sem, aux_sems, auxz_send, auxz_recv, y_send, y_recv, z_send, z_recv, tie_recv,
    kv_send, kv_recv, at_send, at_recv, ay_send, ay_recv, rs_send, rs_recv, ag_send, ag_recv,
):
    row = lax.axis_index("row")
    col = lax.axis_index("col")
    y = row // ZS
    z = row % ZS
    x = col // 2
    core = col % 2
    active = y == core
    partner = {"row": (1 - y) * ZS + z}
    is_owner = jnp.logical_and(active, z % 4 != 3)
    mine = z - z // 4
    head = mine // 2
    half = mine % 2

    def at_z(other):
        return {"row": y * ZS + other}

    def remote(src, dst, send, recv, device):
        return pltpu.make_async_remote_copy(
            src_ref=src, dst_ref=dst, send_sem=send, recv_sem=recv, device_id=device, device_id_type=MESH
        )

    x_load = pltpu.make_async_copy(x_hbm, x_v, load_sem.at[0])
    x_load.start()
    w_loads = [pltpu.make_async_copy(w_hbm.at[j], w_v.at[j], load_sem.at[1 + j]) for j in range(3)]
    for j in ORDER:
        w_loads[j].start()
    gain_load = pltpu.make_async_copy(gain_hbm, gain_v, load_sem.at[5])
    gain_load.start()
    wo_load = pltpu.make_async_copy(wo_hbm, wo_v, load_sem.at[4])
    wo_load.start()

    barrier = pltpu.get_barrier_semaphore()
    pl.semaphore_signal(barrier, inc=1, device_id=partner, device_id_type=MESH)
    for d in range(1, ZS):
        pl.semaphore_signal(barrier, inc=1, device_id=at_z((z + d) % ZS), device_id_type=MESH)
    for d in range(1, COLS):
        pl.semaphore_signal(barrier, inc=1, device_id={"col": (col + d) % COLS}, device_id_type=MESH)

    x_load.wait()
    values = x_v[...].astype(F32)
    mean = jnp.sum(values, axis=1, keepdims=True) * (1.0 / T)
    centered = values - mean
    squares = jnp.sum(centered * centered, axis=1, keepdims=True)
    gain_load.wait()
    gain = gain_v[...].reshape(1, T)
    lhs[0:T, :] = (centered * gain).astype(BF16)
    high = gain.astype(BF16).astype(F32)
    rows = lax.broadcasted_iota(jnp.int32, (16, T), 0)
    lhs[T : T + 16, :] = jnp.where(rows == 0, high, jnp.where(rows == 1, gain - high, 0.0)).astype(BF16)
    lanes = lax.broadcasted_iota(jnp.int32, (T, 128), 1)
    turned = jnp.where(lanes == 0, mean, jnp.where(lanes == 1, squares, 0.0)).T
    early = turned[0:8, :]
    late = pltpu.roll(early, T - HALF, 1)
    for o in range(6):
        source = early if o % 2 == 0 else late
        for r in range(2):
            aux_own[0, o, 3 + 2 * r : 4 + 2 * r, :] = source[r : r + 1, 0:K]
            aux_own[0, o, 4 + 2 * r : 5 + 2 * r, :] = source[r : r + 1, K : 2 * K]

    tie = (z + 4) % ZS
    first = jnp.where(tie % 4 == 3, (tie + 1) % ZS, tie)
    first = first - first // 4

    def order(i):
        return (first + i) % 6

    def y_copy(j, o):
        return remote(y_buf.at[j, o], y_buf.at[j, o], y_send.at[j, o], y_recv.at[j, o], partner)

    aux_copy = remote(aux_own.at[0], aux_own.at[1], aux_sems.at[0], aux_sems.at[1], partner)

    for step, j in enumerate(ORDER):
        w_loads[j].wait()
        product = jnp.dot(lhs[...], w_v[j], preferred_element_type=F32)
        weights_sum = product[T : T + 1, :] + product[T + 1 : T + 2, :]
        for o in range(6):
            aux_own[0, o, j : j + 1, :] = weights_sum[:, (o // 2) * K : (o // 2 + 1) * K]

        @pl.when(active)
        def _():
            for o in range(6):
                part[j, o] = product[(o % 2) * HALF : (o % 2 + 1) * HALF, (o // 2) * K : (o // 2 + 1) * K]

        @pl.when(jnp.logical_not(active))
        def _():
            for o in range(6):
                piece = product[(o % 2) * HALF : (o % 2 + 1) * HALF, (o // 2) * K : (o // 2 + 1) * K]
                y_buf[j, o] = piece.astype(BF16)

        if step == 0:
            pl.semaphore_wait(barrier, 1 + (ZS - 1) + (COLS - 1))

        @pl.when(jnp.logical_not(active))
        def _(step=step):
            if step == 0:
                for i in range(EARLY):
                    y_copy(ORDER[0], order(i)).start()
            if step == 2:
                aux_copy.start()
                for i in range(EARLY, 18):
                    y_copy(ORDER[i // 6], order(i % 6)).start()

    def z_copy(j, o, to):
        return remote(z_buf.at[j, o], z_in.at[z, j], z_send.at[j, o], z_recv.at[z, j], at_z(to))

    def tie_copy(j, o):
        return remote(z_buf.at[j, o], tie_in.at[j], z_send.at[j, o], tie_recv.at[j], at_z((z + 1) % ZS))

    def aux_z_copy(o):
        return remote(aux_own.at[:, o], aux_all.at[z], auxz_send.at[o], auxz_recv.at[z], at_z(owner_z(o)))

    @pl.when(active)
    def _():
        for i in range(18):
            j = ORDER[i // 6]
            o = order(i % 6)
            to = owner_z(o)
            ahead = (to - z + ZS) % ZS

            if i == EARLY:
                aux_copy.wait_recv()
                for owner in range(6):
                    @pl.when(z != owner_z(owner))
                    def _(owner=owner):
                        aux_z_copy(owner).start()

                    @pl.when(z == owner_z(owner))
                    def _(owner=owner):
                        aux_all[z] = aux_own[:, owner]

            y_copy(j, o).wait_recv()
            total = part[j, o] + y_buf[j, o].astype(F32)

            @pl.when(ahead == 0)
            def _(j=j, total=total):
                acc[j] = total

            @pl.when(ahead == 4)
            def _(j=j, o=o, total=total):
                z_buf[j, o] = total.astype(BF16)
                tie_copy(j, o).start()

            @pl.when(ahead == 3)
            def _(i=i, j=j, o=o, to=to, total=total):
                tie_copy(j, o).wait_recv()
                z_buf[j, o] = (total + tie_in[j].astype(F32)).astype(BF16)
                z_copy(j, o, to).start()

            @pl.when(jnp.logical_and(ahead != 0, jnp.logical_and(ahead != 3, ahead != 4)))
            def _(j=j, o=o, to=to, total=total):
                z_buf[j, o] = total.astype(BF16)
                z_copy(j, o, to).start()

    def kv_copy(j):
        return remote(
            qkv.at[j, half], qkv.at[j, half], kv_send.at[j - 1], kv_recv.at[j - 1], at_z(owner_z(mine + 1 - 2 * half))
        )

    def at_copy(o, d):
        return remote(att.at[o], att.at[o], at_send.at[d - 1], at_recv.at[o], at_z((z + d) % ZS))

    def at_forward(o):
        return remote(att.at[o], att.at[o], at_send.at[3], at_recv.at[o], at_z((z + 1) % ZS))

    def ay_copy(o):
        return remote(att.at[o], att.at[o], ay_send.at[o], ay_recv.at[o], partner)

    @pl.when(is_owner)
    def _():
        for d in range(1, ZS):
            other = (z + d) % ZS
            remote(aux_own.at[:, 0], aux_all.at[other], auxz_send.at[0], auxz_recv.at[other], at_z(other)).wait_recv()

        def gathered(r):
            return aux_all[:, :, r, :].reshape(2 * ZS, K)

        means = jnp.concatenate([gathered(3), gathered(4)], axis=1)
        average = jnp.sum(means, axis=0, keepdims=True) * (1.0 / 16)
        offsets = means - average
        sums = jnp.concatenate([gathered(5), gathered(6)], axis=1)
        spread = jnp.sum(sums + T * (offsets * offsets), axis=0, keepdims=True) * (1.0 / FEATURES)
        scale = lax.rsqrt(spread + EPSILON)
        tall = jnp.concatenate([offsets, jnp.broadcast_to(scale, (112, 2 * K))], axis=0).T
        scale_col = tall[0:HALF, 16:17]
        offset_cols = tall[0:HALF, 0:16]

        for j in ORDER:
            total = acc[j] + jnp.dot(
                offset_cols, gathered(j), preferred_element_type=F32, precision=lax.Precision.HIGHEST
            )
            for d in (1, 7, 2, 6, 5, 3):
                other = (z + ZS - d) % ZS
                remote(z_buf.at[j, 0], z_in.at[other, j], z_send.at[0, 0], z_recv.at[other, j], at_z(other)).wait_recv()
                total = total + z_in[other, j].astype(F32)
            qkv[j, half] = (total * scale_col).astype(BF16)
            if j > 0:
                kv_copy(j).start()

        kv_copy(1).wait_recv()
        queries = qkv[0, half]
        keys = qkv[1].reshape(T, K)
        scores = lax.dot_general(
            queries, keys, (((1,), (1,)), ((), ())), preferred_element_type=F32
        ) * (1.0 / math.sqrt(K))
        exponent = jnp.exp(scores - jnp.max(scores, axis=1, keepdims=True))
        weights = (exponent / jnp.sum(exponent, axis=1, keepdims=True)).astype(BF16)
        kv_copy(2).wait_recv()
        mixed = jnp.dot(weights, qkv[2].reshape(T, K), preferred_element_type=F32)
        att[mine] = mixed.astype(BF16)
        for d in (3, 5, 2, 6, 1, 7):
            at_copy(mine, d).start()

    def rs_copy(s, dx):
        there = (x + dx) % 4
        other = 2 * there + s
        return remote(p_buf.at[4 * s + there], p_in.at[col], rs_send.at[s, dx], rs_recv.at[col], {"col": other})

    def wait_load():
        wo_load.wait()

    for s in range(2):
        @pl.when(active)
        def _(s=s):
            for h in range(3):
                o = 2 * h + s

                @pl.when(z != owner_z(o))
                def _(o=o):
                    at_copy(o, 1).wait_recv()

                @pl.when(z == (owner_z(o) + 3) % ZS)
                def _(o=o):
                    at_forward(o).start()

                ay_copy(o).start()

        @pl.when(jnp.logical_not(active))
        def _(s=s):
            for h in range(3):
                ay_copy(2 * h + s).wait_recv()

        if s == 0:
            wait_load()
        attended = jnp.concatenate([att[2 * h + s] for h in range(3)], axis=1)
        product = jnp.dot(attended, wo_v[...], preferred_element_type=F32).astype(BF16)
        for b in range(4):
            p_buf[4 * s + b] = product[b * BLOCK : (b + 1) * BLOCK, :]
        for dx in (2, 1, 3):
            rs_copy(s, dx).start()

        @pl.when(core != s)
        def _(s=s):
            rs_copy(s, 0).start()

    def rows_of(other):
        start = (other % 2) * HALF + (other // 2) * BLOCK
        return o_ref.at[pl.ds(pl.multiple_of(start, BLOCK), BLOCK), :]

    def ag_copy(d):
        return remote(rows_of(col), rows_of(col), ag_send.at[d - 1], ag_recv.at[col], {"col": (col + d) % COLS})

    def from_peers():
        yield 2 * x + 1 - core
        for dx in (1, 3, 2):
            for k in range(2):
                yield 2 * ((x + dx) % 4) + k

    total = p_buf[4 * core + x].astype(F32)
    for n, other in enumerate(from_peers()):
        remote(p_buf.at[0], p_in.at[other], rs_send.at[0, 0], rs_recv.at[other], {"col": other}).wait_recv()
        total = total + p_in[other].astype(F32)
    rows_of(col)[...] = total.astype(BF16)
    for d in range(1, COLS):
        ag_copy(d).start()

    @pl.when(jnp.logical_not(active))
    def _():
        aux_copy.wait_send()
        for j in range(3):
            for o in range(6):
                y_copy(j, o).wait_send()

    @pl.when(active)
    def _():
        for o in range(6):
            ay_copy(o).wait_send()

            @pl.when(z == (owner_z(o) + 3) % ZS)
            def _(o=o):
                at_forward(o).wait_send()

            @pl.when(z != owner_z(o))
            def _(o=o):
                aux_z_copy(o).wait_send()
                for j in range(3):
                    z_copy(j, o, owner_z(o)).wait_send()

    @pl.when(is_owner)
    def _():
        kv_copy(1).wait_send()
        kv_copy(2).wait_send()
        for d in (3, 5, 2, 6, 1, 7):
            at_copy(mine, d).wait_send()

    for s in range(2):
        for dx in range(1, 4):
            rs_copy(s, dx).wait_send()

        @pl.when(core != s)
        def _(s=s):
            rs_copy(s, 0).wait_send()

    for n, other in enumerate(from_peers()):
        remote(rows_of(other), rows_of(other), ag_send.at[0], ag_recv.at[other], {"col": other}).wait_recv()
    for d in range(1, COLS):
        ag_copy(d).wait_send()


def shards(tokens, norm_gain, qkv_weight, out_weight):
    dma = pltpu.SemaphoreType.DMA
    return pl.pallas_call(
        kernel,
        out_shape=pltpu.VMEM((T, T), BF16),
        in_specs=[
            pl.BlockSpec(memory_space=pl.ANY),
            pl.BlockSpec(memory_space=pl.ANY),
            pl.BlockSpec(memory_space=pl.ANY),
            pl.BlockSpec(memory_space=pl.ANY),
        ],
        out_specs=pl.BlockSpec(memory_space=pltpu.VMEM),
        scratch_shapes=[
            pltpu.VMEM((T, T), BF16),
            pltpu.VMEM((T,), F32),
            pltpu.VMEM((3, T, T), BF16),
            pltpu.VMEM((T, T), BF16),
            pltpu.VMEM((T + 16, T), BF16),
            pltpu.VMEM((2, 6, 8, K), F32),
            pltpu.VMEM((ZS, 2, 8, K), F32),
            pltpu.VMEM((3, 6, HALF, K), F32),
            pltpu.VMEM((3, 6, HALF, K), BF16),
            pltpu.VMEM((3, 6, HALF, K), BF16),
            pltpu.VMEM((ZS, 3, HALF, K), BF16),
            pltpu.VMEM((3, HALF, K), BF16),
            pltpu.VMEM((3, HALF, K), F32),
            pltpu.VMEM((3, 2, HALF, K), BF16),
            pltpu.VMEM((6, HALF, K), BF16),
            pltpu.VMEM((COLS, BLOCK, T), BF16),
            pltpu.VMEM((COLS, BLOCK, T), BF16),
            dma((6,)),
            dma((2,)),
            dma((6,)),
            dma((ZS,)),
            dma((3, 6)),
            dma((3, 6)),
            dma((3, 6)),
            dma((ZS, 3)),
            dma((3,)),
            dma((2,)),
            dma((2,)),
            dma((ZS - 1,)),
            dma((6,)),
            dma((6,)),
            dma((6,)),
            dma((2, 4)),
            dma((COLS,)),
            dma((COLS - 1,)),
            dma((COLS,)),
        ],
        compiler_params=pltpu.CompilerParams(collective_id=0, has_side_effects=True),
        name="sublayer",
    )(tokens, norm_gain, jnp.transpose(qkv_weight, (1, 0, 2)), out_weight)


def solution(mesh):
    in_specs = (P("dp", "row"), P("row"), P("row", None, "col"), P("col", "row"))
    out_specs = P("dp", "row")
    return jax.shard_map(shards, mesh=mesh, in_specs=in_specs, out_specs=out_specs, check_vma=False)
```

```python
import math

import jax
import jax.numpy as jnp
from jax import lax
from jax.experimental import pallas as pl
from jax.experimental.pallas import tpu as pltpu
from jax.sharding import PartitionSpec as P

K = 128
EPSILON = 1e-05
F32 = jnp.float32
BF16 = jnp.bfloat16
T = 384
HALF = 192
BLOCK = 48
ZS = 8
XS = 4
FEATURES = 6144
ORDER = (2, 1, 0)
EARLY = 2
MESH = pl.DeviceIdType.MESH


def owner_z(owner):
    return owner + owner // 3


def kernel(
    x_hbm, gain_hbm, w_hbm, wo_hbm, o_ref,
    x_v, gain_v, w_v, wo_v, lhs, aux_own, aux_all, part, y_buf, z_buf, z_in, tie_in, acc, v_out, v_in, qkv, att,
    pair_out, pair_in, p_buf, p_in,
    load_sem, aux_sems, auxz_send, auxz_recv, y_send, y_recv, z_send, z_recv, tie_recv, v_sems,
    kv_send, kv_recv, at_send, at_recv, ay_send, ay_recv, pair_sems, rs_sems, ag_send, ag_recv,
):
    row = lax.axis_index("row")
    col = lax.axis_index("col")
    y = row // ZS
    z = row % ZS
    x = col // 2
    core = col % 2
    active = y == core
    partner = {"row": (1 - y) * ZS + z}
    pair = {"col": 2 * x + 1 - core}
    owns = z % 4 != 3
    is_owner = jnp.logical_and(active, owns)
    mine = z - z // 4
    head = mine // 2
    half = mine % 2

    def at_x(d):
        return {"col": 2 * ((x + d) % XS) + core}

    def at_z(other):
        return {"row": y * ZS + other}

    def remote(src, dst, send, recv, device):
        return pltpu.make_async_remote_copy(
            src_ref=src, dst_ref=dst, send_sem=send, recv_sem=recv, device_id=device, device_id_type=MESH
        )

    x_load = pltpu.make_async_copy(x_hbm, x_v, load_sem.at[0])
    x_load.start()
    w_loads = [pltpu.make_async_copy(w_hbm.at[j], w_v.at[j], load_sem.at[1 + j]) for j in range(3)]
    for j in ORDER:
        w_loads[j].start()
    gain_load = pltpu.make_async_copy(gain_hbm, gain_v, load_sem.at[5])
    gain_load.start()
    wo_load = pltpu.make_async_copy(wo_hbm, wo_v, load_sem.at[4])
    wo_load.start()

    barrier = pltpu.get_barrier_semaphore()
    pl.semaphore_signal(barrier, inc=1, device_id=partner, device_id_type=MESH)
    pl.semaphore_signal(barrier, inc=1, device_id=pair, device_id_type=MESH)
    for d in range(1, XS):
        pl.semaphore_signal(barrier, inc=1, device_id=at_x(d), device_id_type=MESH)
    pl.semaphore_signal(barrier, inc=1, device_id=at_z((z + 7) % ZS), device_id_type=MESH)

    @pl.when(owns)
    def _():
        for d in range(1, ZS - 1):
            pl.semaphore_signal(barrier, inc=1, device_id=at_z((z + d) % ZS), device_id_type=MESH)

    arrivals = 5 + jnp.where(owns, 5, 6) + jnp.where(z % 4 == 2, 1, 0)

    x_load.wait()
    values = x_v[...].astype(F32)
    mean = jnp.sum(values, axis=1, keepdims=True) * (1.0 / T)
    centered = values - mean
    squares = jnp.sum(centered * centered, axis=1, keepdims=True)
    gain_load.wait()
    gain = gain_v[...].reshape(1, T)
    lhs[0:T, :] = (centered * gain).astype(BF16)
    high = gain.astype(BF16).astype(F32)
    rows = lax.broadcasted_iota(jnp.int32, (16, T), 0)
    lhs[T : T + 16, :] = jnp.where(rows == 0, high, jnp.where(rows == 1, gain - high, 0.0)).astype(BF16)
    lanes = lax.broadcasted_iota(jnp.int32, (T, 128), 1)
    turned = jnp.where(lanes == 0, mean, jnp.where(lanes == 1, squares, 0.0)).T
    early = turned[0:8, :]
    late = pltpu.roll(early, T - HALF, 1)
    for o in range(6):
        source = early if o % 2 == 0 else late
        for r in range(2):
            aux_own[0, o, 3 + 2 * r : 4 + 2 * r, :] = source[r : r + 1, 0:K]
            aux_own[0, o, 4 + 2 * r : 5 + 2 * r, :] = source[r : r + 1, K : 2 * K]

    tie = (z + 4) % ZS
    first = jnp.where(tie % 4 == 3, (tie + 1) % ZS, tie)
    first = first - first // 4

    def order(i):
        return (first + i) % 6

    def y_copy(n, o):
        return remote(y_buf.at[n, o], y_buf.at[n, o], y_send.at[0], y_recv.at[n, o], partner)

    aux_copy = remote(aux_own.at[0], aux_own.at[1], aux_sems.at[0], aux_sems.at[1], partner)

    def z_copy(j, o, to):
        return remote(z_buf.at[j, o], z_in.at[z, j], z_send.at[0], z_recv.at[j], at_z(to))

    def tie_copy(j, o):
        return remote(z_buf.at[j, o], tie_in.at[j], z_send.at[0], tie_recv.at[j], at_z((z + 1) % ZS))

    def aux_z_copy(o):
        return remote(aux_own.at[:, o], aux_all.at[z], auxz_send.at[0], auxz_recv.at[0], at_z(owner_z(o)))

    def z_send_piece(j, o, total, with_tie):
        to = owner_z(o)
        ahead = (to - z + ZS) % ZS

        @pl.when(ahead == 0)
        def _():
            acc[j] = total

        @pl.when(ahead == 4)
        def _():
            z_buf[j, o] = total.astype(BF16)
            tie_copy(j, o).start()

        if with_tie:
            @pl.when(ahead == 3)
            def _():
                tie_copy(j, o).wait_recv()
                z_buf[j, o] = (total + tie_in[j].astype(F32)).astype(BF16)
                z_copy(j, o, to).start()

        @pl.when(jnp.logical_and(ahead != 0, jnp.logical_and(ahead != 3, ahead != 4)))
        def _():
            z_buf[j, o] = total.astype(BF16)
            z_copy(j, o, to).start()

    for step, j in enumerate(ORDER):
        w_loads[j].wait()
        product = jnp.dot(lhs[...], w_v[j], preferred_element_type=F32)
        weights_sum = product[T : T + 1, :] + product[T + 1 : T + 2, :]
        for o in range(6):
            aux_own[0, o, j : j + 1, :] = weights_sum[:, (o // 2) * K : (o // 2 + 1) * K]

        def piece(o):
            return product[(o % 2) * HALF : (o % 2 + 1) * HALF, (o // 2) * K : (o // 2 + 1) * K]

        if step == 0:
            for o in range(6):
                part[j, o] = piece(o)
            pl.semaphore_wait(barrier, arrivals)
            for i in range(6):
                o = order(i)
                z_send_piece(j, o, part[j, o], False)
        else:
            @pl.when(active)
            def _():
                for o in range(6):
                    part[j, o] = piece(o)

            @pl.when(jnp.logical_not(active))
            def _(step=step):
                for o in range(6):
                    y_buf[step - 1, o] = piece(o).astype(BF16)
                if step == 1:
                    for i in range(EARLY):
                        y_copy(0, order(i)).start()
                else:
                    aux_copy.start()
                    for i in range(EARLY, 12):
                        y_copy(i // 6, order(i % 6)).start()

    @pl.when(z % 4 != 0)
    def _():
        o = order(5)
        tie_copy(2, o).wait_recv()
        z_buf[2, o] = (part[2, o] + tie_in[2].astype(F32)).astype(BF16)
        z_copy(2, o, (z + 3) % ZS).start()

    @pl.when(active)
    def _():
        for i in range(12):
            n = i // 6
            j = ORDER[1 + n]
            o = order(i % 6)

            if i == EARLY:
                aux_copy.wait_recv()
                for owner in range(6):
                    @pl.when(z != owner_z(owner))
                    def _(owner=owner):
                        aux_z_copy(owner).start()

                    @pl.when(z == owner_z(owner))
                    def _(owner=owner):
                        aux_all[z] = aux_own[:, owner]

            y_copy(n, o).wait_recv()
            z_send_piece(j, o, part[j, o] + y_buf[n, o].astype(F32), True)

    def kv_copy(j):
        return remote(
            qkv.at[j, half], qkv.at[j, half], kv_send.at[j - 1], kv_recv.at[j - 1], at_z(owner_z(mine + 1 - 2 * half))
        )

    def at_copy(d):
        return remote(att.at[mine], att.at[mine], at_send.at[0], at_recv.at[mine], at_z((z + d) % ZS))

    def at_forward(o):
        return remote(att.at[o], att.at[o], at_send.at[1], at_recv.at[o], at_z((z + 1) % ZS))

    def ay_copy(o):
        return remote(att.at[o], att.at[o], ay_send.at[0], ay_recv.at[o], partner)

    v_copy = remote(v_out, v_in, v_sems.at[0], v_sems.at[1], partner)

    def summed(j, start):
        remote(z_in.at[pl.ds(0, 6), 0], z_in.at[pl.ds(0, 6), j], z_send.at[0], z_recv.at[j], partner).wait_recv()
        total = start
        for d in (1, 7, 2, 6, 5, 3):
            total = total + z_in[(z + ZS - d) % ZS, j].astype(F32)
        return total

    @pl.when(jnp.logical_and(jnp.logical_not(active), owns))
    def _():
        v_out[...] = summed(2, acc[2]).astype(BF16)
        v_copy.start()

    @pl.when(is_owner)
    def _():
        remote(
            aux_all.at[pl.ds(0, 7)], aux_all.at[pl.ds(0, 7)], auxz_send.at[0], auxz_recv.at[0], partner
        ).wait_recv()

        def gathered(r):
            return aux_all[:, :, r, :].reshape(2 * ZS, K)

        means = jnp.concatenate([gathered(3), gathered(4)], axis=1)
        average = jnp.sum(means, axis=0, keepdims=True) * (1.0 / 16)
        offsets = means - average
        sums = jnp.concatenate([gathered(5), gathered(6)], axis=1)
        spread = jnp.sum(sums + T * (offsets * offsets), axis=0, keepdims=True) * (1.0 / FEATURES)
        scale = lax.rsqrt(spread + EPSILON)
        tall = jnp.concatenate([offsets, jnp.broadcast_to(scale, (112, 2 * K))], axis=0).T
        scale_col = tall[0:HALF, 16:17]
        offset_cols = tall[0:HALF, 0:16]

        for j in ORDER:
            start = acc[j] + jnp.dot(
                offset_cols, gathered(j), preferred_element_type=F32, precision=lax.Precision.HIGHEST
            )
            if j == 2:
                v_copy.wait_recv()
                start = start + v_in[...].astype(F32)
            qkv[j, half] = (summed(j, start) * scale_col).astype(BF16)
            if j > 0:
                kv_copy(j).start()

        kv_copy(1).wait_recv()
        queries = qkv[0, half]
        keys = qkv[1].reshape(T, K)
        scores = lax.dot_general(
            queries, keys, (((1,), (1,)), ((), ())), preferred_element_type=F32
        ) * (1.0 / math.sqrt(K))
        exponent = jnp.exp(scores - jnp.max(scores, axis=1, keepdims=True))
        weights = (exponent / jnp.sum(exponent, axis=1, keepdims=True)).astype(BF16)
        kv_copy(2).wait_recv()
        mixed = jnp.dot(weights, qkv[2].reshape(T, K), preferred_element_type=F32)
        att[mine] = mixed.astype(BF16)
        for d in (3, 5, 2, 6, 1, 7):
            at_copy(d).start()

    pair_copy = remote(pair_out, pair_in, pair_sems.at[0], pair_sems.at[1], pair)

    def rs_copy(d):
        return remote(p_buf.at[(x + d) % XS], p_in.at[x], rs_sems.at[0], rs_sems.at[1], at_x(d))

    for n in range(2):
        s = jnp.where(n == 0, 1 - core, core)

        @pl.when(active)
        def _(s=s, n=n):
            for h in range(3):
                o = 2 * h + s

                @pl.when(z != owner_z(o))
                def _(o=o, h=h):
                    remote(att.at[o], att.at[o], at_send.at[0], at_recv.at[o], partner).wait_recv()

                @pl.when(z == (owner_z(o) + 3) % ZS)
                def _(o=o):
                    at_forward(o).start()

                ay_copy(o).start()

        @pl.when(jnp.logical_not(active))
        def _(s=s, n=n):
            for h in range(3):
                ay_copy(2 * h + s).wait_recv()

        if n == 0:
            wo_load.wait()
        attended = jnp.concatenate([att[2 * h + s] for h in range(3)], axis=1)
        product = jnp.dot(attended, wo_v[...], preferred_element_type=F32)
        if n == 0:
            pair_out[...] = product.astype(BF16)
            pair_copy.start()
        else:
            pair_copy.wait_recv()
            both = (product + pair_in[...].astype(F32)).astype(BF16)
            for b in range(XS):
                p_buf[b] = both[b * BLOCK : (b + 1) * BLOCK, :]
            for d in (2, 1, 3):
                rs_copy(d).start()

    def rows_of(k, b):
        return o_ref.at[pl.ds(pl.multiple_of(k * HALF + b * BLOCK, BLOCK), BLOCK), :]

    def ag_copy(b, n, device):
        rows = rows_of(core, b)
        return remote(rows, rows, ag_send.at[n], ag_recv.at[core, b], device)

    remote(p_in.at[pl.ds(0, 3)], p_in.at[pl.ds(0, 3)], rs_sems.at[0], rs_sems.at[1], pair).wait_recv()
    total = p_buf[x].astype(F32)
    for d in (1, 3, 2):
        total = total + p_in[(x + d) % XS].astype(F32)
    rows_of(core, x)[...] = total.astype(BF16)
    for d in (2, 1, 3):
        ag_copy(x, 0, at_x(d)).start()
    ag_copy(x, 1, pair).start()

    def sent(ref, sem):
        remote(ref, ref, sem, sem, pair).wait_send()

    @pl.when(jnp.logical_not(active))
    def _():
        aux_copy.wait_send()
        sent(y_buf, y_send.at[0])

        @pl.when(owns)
        def _():
            v_copy.wait_send()
            sent(z_buf.at[0, pl.ds(0, 5)], z_send.at[0])

        @pl.when(jnp.logical_not(owns))
        def _():
            sent(z_buf.at[0], z_send.at[0])

    @pl.when(active)
    def _():
        sent(att, ay_send.at[0])

        @pl.when(z % 4 != 2)
        def _():
            sent(att.at[0], at_send.at[1])

        @pl.when(owns)
        def _():
            sent(aux_all.at[pl.ds(0, 5)], auxz_send.at[0])
            sent(z_buf.at[:, pl.ds(0, 5)], z_send.at[0])
            kv_copy(1).wait_send()
            kv_copy(2).wait_send()
            sent(att, at_send.at[0])

        @pl.when(jnp.logical_not(owns))
        def _():
            sent(aux_all.at[pl.ds(0, 6)], auxz_send.at[0])
            sent(z_buf, z_send.at[0])

    pair_copy.wait_send()
    sent(p_in.at[pl.ds(0, 3)], rs_sems.at[0])

    for d in (1, 3, 2):
        b = (x + d) % XS
        ag_copy(b, 0, pair).wait_recv()
        ag_copy(b, 1, pair).start()
    for d in (0, 1, 3, 2):
        b = (x + d) % XS
        remote(rows_of(1 - core, b), rows_of(1 - core, b), ag_send.at[0], ag_recv.at[1 - core, b], pair).wait_recv()
    sent(o_ref.at[pl.ds(0, 3 * BLOCK), :], ag_send.at[0])
    sent(o_ref.at[pl.ds(0, 4 * BLOCK), :], ag_send.at[1])


def shards(tokens, norm_gain, qkv_weight, out_weight):
    dma = pltpu.SemaphoreType.DMA
    return pl.pallas_call(
        kernel,
        out_shape=pltpu.VMEM((T, T), BF16),
        in_specs=[
            pl.BlockSpec(memory_space=pl.ANY),
            pl.BlockSpec(memory_space=pl.ANY),
            pl.BlockSpec(memory_space=pl.ANY),
            pl.BlockSpec(memory_space=pl.ANY),
        ],
        out_specs=pl.BlockSpec(memory_space=pltpu.VMEM),
        scratch_shapes=[
            pltpu.VMEM((T, T), BF16),
            pltpu.VMEM((T,), F32),
            pltpu.VMEM((3, T, T), BF16),
            pltpu.VMEM((T, T), BF16),
            pltpu.VMEM((T + 16, T), BF16),
            pltpu.VMEM((2, 6, 8, K), F32),
            pltpu.VMEM((ZS, 2, 8, K), F32),
            pltpu.VMEM((3, 6, HALF, K), F32),
            pltpu.VMEM((2, 6, HALF, K), BF16),
            pltpu.VMEM((3, 6, HALF, K), BF16),
            pltpu.VMEM((ZS, 3, HALF, K), BF16),
            pltpu.VMEM((3, HALF, K), BF16),
            pltpu.VMEM((3, HALF, K), F32),
            pltpu.VMEM((HALF, K), BF16),
            pltpu.VMEM((HALF, K), BF16),
            pltpu.VMEM((3, 2, HALF, K), BF16),
            pltpu.VMEM((6, HALF, K), BF16),
            pltpu.VMEM((HALF, T), BF16),
            pltpu.VMEM((HALF, T), BF16),
            pltpu.VMEM((XS, BLOCK, T), BF16),
            pltpu.VMEM((XS, BLOCK, T), BF16),
            dma((6,)),
            dma((2,)),
            dma((1,)),
            dma((1,)),
            dma((1,)),
            dma((2, 6)),
            dma((1,)),
            dma((3,)),
            dma((3,)),
            dma((2,)),
            dma((2,)),
            dma((2,)),
            dma((2,)),
            dma((6,)),
            dma((1,)),
            dma((6,)),
            dma((2,)),
            dma((2,)),
            dma((2,)),
            dma((2, XS)),
        ],
        compiler_params=pltpu.CompilerParams(collective_id=0, has_side_effects=True),
        name="sublayer",
    )(tokens, norm_gain, jnp.transpose(qkv_weight, (1, 0, 2)), out_weight)


def solution(mesh):
    in_specs = (P("dp", "row"), P("row"), P("row", None, "col"), P("col", "row"))
    out_specs = P("dp", "row")
    return jax.shard_map(shards, mesh=mesh, in_specs=in_specs, out_specs=out_specs, check_vma=False)
```

```python
import math

import jax
import jax.numpy as jnp
from jax import lax
from jax.experimental import pallas as pl
from jax.experimental.pallas import tpu as pltpu
from jax.sharding import PartitionSpec as P

K = 128
EPSILON = 1e-05
F32 = jnp.float32
BF16 = jnp.bfloat16
T = 384
HALF = 192
BLOCK = 48
ZS = 8
XS = 4
FEATURES = 6144
ORDER = (2, 1, 0)
CHAINS = ((4, 5, 6, 2, 1, 0), (4, 5, 3, 7, 1, 0), (4, 3, 6, 2, 7, 0), (5, 3, 6, 2, 7, 1))
MESH = pl.DeviceIdType.MESH


def owner_z(owner):
    return owner + owner // 3


def kernel(
    x_hbm, gain_hbm, w_hbm, wo_hbm, o_ref,
    x_v, gain_v, w_v, wo_v, lhs, aux_own, aux_all, part, y_buf, z_buf, plus_in, minus_in, acc, v_out, v_in, qkv, att,
    pair_out, pair_in, p_buf, p_in,
    load_sem, aux_sems, auxz_send, auxz_recv, y_send, y_recv, z_send, plus_recv, minus_recv, v_sems,
    kv_send, kv_recv, at_send, at_recv, ay_send, ay_recv, pair_sems, rs_sems, ag_send, ag_recv,
):
    row = lax.axis_index("row")
    col = lax.axis_index("col")
    y = row // ZS
    z = row % ZS
    x = col // 2
    core = col % 2
    active = y == core
    partner = {"row": (1 - y) * ZS + z}
    pair = {"col": 2 * x + 1 - core}
    owns = z % 4 != 3
    is_owner = jnp.logical_and(active, owns)
    mine = z - z // 4
    head = mine // 2
    half = mine % 2

    def at_x(d):
        return {"col": 2 * ((x + d) % XS) + core}

    def at_z(other):
        return {"row": y * ZS + other}

    def remote(src, dst, send, recv, device):
        return pltpu.make_async_remote_copy(
            src_ref=src, dst_ref=dst, send_sem=send, recv_sem=recv, device_id=device, device_id_type=MESH
        )

    x_load = pltpu.make_async_copy(x_hbm, x_v, load_sem.at[0])
    x_load.start()
    w_loads = [pltpu.make_async_copy(w_hbm.at[j], w_v.at[j], load_sem.at[1 + j]) for j in range(3)]
    for j in ORDER:
        w_loads[j].start()
    gain_load = pltpu.make_async_copy(gain_hbm, gain_v, load_sem.at[5])
    gain_load.start()
    wo_load = pltpu.make_async_copy(wo_hbm, wo_v, load_sem.at[4])
    wo_load.start()

    barrier = pltpu.get_barrier_semaphore()
    pl.semaphore_signal(barrier, inc=1, device_id=partner, device_id_type=MESH)
    pl.semaphore_signal(barrier, inc=1, device_id=pair, device_id_type=MESH)
    for d in range(1, XS):
        pl.semaphore_signal(barrier, inc=1, device_id=at_x(d), device_id_type=MESH)
    pl.semaphore_signal(barrier, inc=1, device_id=at_z((z + 7) % ZS), device_id_type=MESH)

    pl.semaphore_signal(barrier, inc=1, device_id=at_z((z + 1) % ZS), device_id_type=MESH)

    @pl.when(owns)
    def _():
        for d in range(2, ZS - 1):
            pl.semaphore_signal(barrier, inc=1, device_id=at_z((z + d) % ZS), device_id_type=MESH)

    arrivals = 5 + jnp.where(owns, 5, 6) + jnp.where(z % 2 == 0, 1, 0)

    x_load.wait()
    values = x_v[...].astype(F32)
    mean = jnp.sum(values, axis=1, keepdims=True) * (1.0 / T)
    centered = values - mean
    squares = jnp.sum(centered * centered, axis=1, keepdims=True)
    gain_load.wait()
    gain = gain_v[...].reshape(1, T)
    lhs[0:T, :] = (centered * gain).astype(BF16)
    high = gain.astype(BF16).astype(F32)
    rows = lax.broadcasted_iota(jnp.int32, (16, T), 0)
    lhs[T : T + 16, :] = jnp.where(rows == 0, high, jnp.where(rows == 1, gain - high, 0.0)).astype(BF16)
    lanes = lax.broadcasted_iota(jnp.int32, (T, 128), 1)
    turned = jnp.where(lanes == 0, mean, jnp.where(lanes == 1, squares, 0.0)).T
    early = turned[0:8, :]
    late = pltpu.roll(early, T - HALF, 1)
    for o in range(6):
        source = early if o % 2 == 0 else late
        for r in range(2):
            aux_own[0, o, 3 + 2 * r : 4 + 2 * r, :] = source[r : r + 1, 0:K]
            aux_own[0, o, 4 + 2 * r : 5 + 2 * r, :] = source[r : r + 1, K : 2 * K]

    kind = z % 4

    def ahead_of(i):
        steps = [chain[i] for chain in CHAINS]
        return jnp.where(kind == 0, steps[0], jnp.where(kind == 1, steps[1], jnp.where(kind == 2, steps[2], steps[3])))

    aheads = [ahead_of(i) for i in range(6)]

    def order(i):
        to = (z + aheads[i]) % ZS
        return to - to // 4

    def y_copy(n, o):
        return remote(y_buf.at[n, o], y_buf.at[n, o], y_send.at[0], y_recv.at[n, o], partner)

    aux_copy = remote(aux_own.at[0], aux_own.at[1], aux_sems.at[0], aux_sems.at[1], partner)

    def plus_copy(j, o, ahead):
        return remote(z_buf.at[j, o], plus_in.at[j, ahead - 1], z_send.at[0], plus_recv.at[j, ahead - 1], at_z((z + 1) % ZS))

    def minus_copy(j, o, ahead):
        return remote(z_buf.at[j, o], minus_in.at[j, 7 - ahead], z_send.at[0], minus_recv.at[j, 7 - ahead], at_z((z + 7) % ZS))

    def plus_arrived(j, ahead):
        remote(z_buf.at[j, 0], plus_in.at[j, ahead], z_send.at[0], plus_recv.at[j, ahead], partner).wait_recv()
        return plus_in[j, ahead].astype(F32)

    def minus_arrived(j, behind):
        remote(z_buf.at[j, 0], minus_in.at[j, behind], z_send.at[0], minus_recv.at[j, behind], partner).wait_recv()
        return minus_in[j, behind].astype(F32)

    def aux_z_copy(o):
        return remote(aux_own.at[:, o], aux_all.at[z], auxz_send.at[0], auxz_recv.at[0], at_z(owner_z(o)))

    def z_step(j, i):
        o = order(i)
        ahead = aheads[i]

        def term():
            if j == 2:
                return part[j, o]
            return part[j, o] + y_buf[1 - j, o].astype(F32)

        if j != 2:
            y_copy(1 - j, o).wait_recv()

        @pl.when(ahead == 0)
        def _():
            acc[j] = term()

        @pl.when(ahead == 4)
        def _():
            z_buf[j, o] = term().astype(BF16)
            plus_copy(j, o, ahead).start()

        @pl.when(ahead == 5)
        def _():
            z_buf[j, o] = term().astype(BF16)
            minus_copy(j, o, ahead).start()

        @pl.when(jnp.logical_and(ahead > 0, ahead < 4))
        def _():
            before = plus_arrived(j, ahead)
            z_buf[j, o] = (before + term()).astype(BF16)
            plus_copy(j, o, ahead).start()

        @pl.when(ahead > 5)
        def _():
            before = minus_arrived(j, 8 - ahead)
            z_buf[j, o] = (before + term()).astype(BF16)
            minus_copy(j, o, ahead).start()

    for step, j in enumerate(ORDER):
        w_loads[j].wait()
        product = jnp.dot(lhs[...], w_v[j], preferred_element_type=F32)
        weights_sum = product[T : T + 1, :] + product[T + 1 : T + 2, :]
        for o in range(6):
            aux_own[0, o, j : j + 1, :] = weights_sum[:, (o // 2) * K : (o // 2 + 1) * K]

        def piece(o):
            return product[(o % 2) * HALF : (o % 2 + 1) * HALF, (o // 2) * K : (o // 2 + 1) * K]

        if step == 0:
            for o in range(6):
                part[j, o] = piece(o)
            pl.semaphore_wait(barrier, arrivals)
            for i in range(2):
                z_step(j, i)
        else:
            @pl.when(active)
            def _():
                for o in range(6):
                    part[j, o] = piece(o)

            @pl.when(jnp.logical_not(active))
            def _(step=step):
                for o in range(6):
                    y_buf[step - 1, o] = piece(o).astype(BF16)
                if step == 1:
                    y_copy(0, order(0)).start()
                else:
                    y_copy(1, order(0)).start()
                    aux_copy.start()
                    for i in range(1, 6):
                        for n in range(2):
                            y_copy(n, order(i)).start()

    @pl.when(jnp.logical_not(active))
    def _():
        for i in range(2, 6):
            z_step(2, i)

    @pl.when(active)
    def _():
        z_step(2, 2)
        z_step(1, 0)
        z_step(0, 0)
        aux_copy.wait_recv()
        for owner in range(6):
            @pl.when(z != owner_z(owner))
            def _(owner=owner):
                aux_z_copy(owner).start()

            @pl.when(z == owner_z(owner))
            def _(owner=owner):
                aux_all[z] = aux_own[:, owner]

        for j, i in ((1, 1), (0, 1), (2, 3), (1, 2), (0, 2), (2, 4), (1, 3), (0, 3), (2, 5), (1, 4), (0, 4), (1, 5), (0, 5)):
            z_step(j, i)

    def kv_copy(j):
        return remote(
            qkv.at[j, half], qkv.at[j, half], kv_send.at[j - 1], kv_recv.at[j - 1], at_z(owner_z(mine + 1 - 2 * half))
        )

    def at_copy(d):
        return remote(att.at[mine], att.at[mine], at_send.at[0], at_recv.at[mine], at_z((z + d) % ZS))

    def at_forward(o):
        return remote(att.at[o], att.at[o], at_send.at[1], at_recv.at[o], at_z((z + 1) % ZS))

    def ay_copy(o):
        return remote(att.at[o], att.at[o], ay_send.at[0], ay_recv.at[o], partner)

    v_copy = remote(v_out, v_in, v_sems.at[0], v_sems.at[1], partner)

    def summed(j, start):
        total = start + plus_arrived(j, 0)
        total = total + minus_arrived(j, 0)
        return total

    @pl.when(jnp.logical_and(jnp.logical_not(active), owns))
    def _():
        v_out[...] = summed(2, acc[2]).astype(BF16)
        v_copy.start()

    @pl.when(is_owner)
    def _():
        remote(
            aux_all.at[pl.ds(0, 7)], aux_all.at[pl.ds(0, 7)], auxz_send.at[0], auxz_recv.at[0], partner
        ).wait_recv()

        def gathered(r):
            return aux_all[:, :, r, :].reshape(2 * ZS, K)

        means = jnp.concatenate([gathered(3), gathered(4)], axis=1)
        average = jnp.sum(means, axis=0, keepdims=True) * (1.0 / 16)
        offsets = means - average
        sums = jnp.concatenate([gathered(5), gathered(6)], axis=1)
        spread = jnp.sum(sums + T * (offsets * offsets), axis=0, keepdims=True) * (1.0 / FEATURES)
        scale = lax.rsqrt(spread + EPSILON)
        tall = jnp.concatenate([offsets, jnp.broadcast_to(scale, (112, 2 * K))], axis=0).T
        scale_col = tall[0:HALF, 16:17]
        offset_cols = tall[0:HALF, 0:16]

        for j in ORDER:
            start = acc[j] + jnp.dot(
                offset_cols, gathered(j), preferred_element_type=F32, precision=lax.Precision.HIGHEST
            )
            if j == 2:
                v_copy.wait_recv()
                start = start + v_in[...].astype(F32)
            qkv[j, half] = (summed(j, start) * scale_col).astype(BF16)
            if j > 0:
                kv_copy(j).start()

        kv_copy(1).wait_recv()
        queries = qkv[0, half]
        keys = qkv[1].reshape(T, K)
        scores = lax.dot_general(
            queries, keys, (((1,), (1,)), ((), ())), preferred_element_type=F32
        ) * (1.0 / math.sqrt(K))
        exponent = jnp.exp(scores - jnp.max(scores, axis=1, keepdims=True))
        weights = (exponent / jnp.sum(exponent, axis=1, keepdims=True)).astype(BF16)
        kv_copy(2).wait_recv()
        mixed = jnp.dot(weights, qkv[2].reshape(T, K), preferred_element_type=F32)
        att[mine] = mixed.astype(BF16)
        for d in (3, 5, 2, 6, 1, 7):
            at_copy(d).start()

    pair_copy = remote(pair_out, pair_in, pair_sems.at[0], pair_sems.at[1], pair)

    def rs_copy(d):
        return remote(p_buf.at[(x + d) % XS], p_in.at[x], rs_sems.at[0], rs_sems.at[1], at_x(d))

    for n in range(2):
        s = jnp.where(n == 0, 1 - core, core)

        @pl.when(active)
        def _(s=s, n=n):
            for h in range(3):
                o = 2 * h + s

                @pl.when(z != owner_z(o))
                def _(o=o, h=h):
                    remote(att.at[o], att.at[o], at_send.at[0], at_recv.at[o], partner).wait_recv()

                @pl.when(z == (owner_z(o) + 3) % ZS)
                def _(o=o):
                    at_forward(o).start()

                ay_copy(o).start()

        @pl.when(jnp.logical_not(active))
        def _(s=s, n=n):
            for h in range(3):
                ay_copy(2 * h + s).wait_recv()

        if n == 0:
            wo_load.wait()
        attended = jnp.concatenate([att[2 * h + s] for h in range(3)], axis=1)
        product = jnp.dot(attended, wo_v[...], preferred_element_type=F32)
        if n == 0:
            pair_out[...] = product.astype(BF16)
            pair_copy.start()
        else:
            pair_copy.wait_recv()
            both = (product + pair_in[...].astype(F32)).astype(BF16)
            for b in range(XS):
                p_buf[b] = both[b * BLOCK : (b + 1) * BLOCK, :]
            for d in (2, 1, 3):
                rs_copy(d).start()

    def rows_of(k, b):
        return o_ref.at[pl.ds(pl.multiple_of(k * HALF + b * BLOCK, BLOCK), BLOCK), :]

    def ag_copy(b, n, device):
        rows = rows_of(core, b)
        return remote(rows, rows, ag_send.at[n], ag_recv.at[core, b], device)

    remote(p_in.at[pl.ds(0, 3)], p_in.at[pl.ds(0, 3)], rs_sems.at[0], rs_sems.at[1], pair).wait_recv()
    total = p_buf[x].astype(F32)
    for d in (1, 3, 2):
        total = total + p_in[(x + d) % XS].astype(F32)
    rows_of(core, x)[...] = total.astype(BF16)
    for d in (2, 1, 3):
        ag_copy(x, 0, at_x(d)).start()
    ag_copy(x, 1, pair).start()

    def sent(ref, sem):
        remote(ref, ref, sem, sem, pair).wait_send()

    @pl.when(jnp.logical_not(active))
    def _():
        aux_copy.wait_send()
        sent(y_buf, y_send.at[0])

        @pl.when(owns)
        def _():
            v_copy.wait_send()
            sent(z_buf.at[0, pl.ds(0, 5)], z_send.at[0])

        @pl.when(jnp.logical_not(owns))
        def _():
            sent(z_buf.at[0], z_send.at[0])

    @pl.when(active)
    def _():
        sent(att, ay_send.at[0])

        @pl.when(z % 4 != 2)
        def _():
            sent(att.at[0], at_send.at[1])

        @pl.when(owns)
        def _():
            sent(aux_all.at[pl.ds(0, 5)], auxz_send.at[0])
            sent(z_buf.at[:, pl.ds(0, 5)], z_send.at[0])
            kv_copy(1).wait_send()
            kv_copy(2).wait_send()
            sent(att, at_send.at[0])

        @pl.when(jnp.logical_not(owns))
        def _():
            sent(aux_all.at[pl.ds(0, 6)], auxz_send.at[0])
            sent(z_buf, z_send.at[0])

    pair_copy.wait_send()
    sent(p_in.at[pl.ds(0, 3)], rs_sems.at[0])

    for d in (1, 3, 2):
        b = (x + d) % XS
        ag_copy(b, 0, pair).wait_recv()
        ag_copy(b, 1, pair).start()
    for d in (0, 1, 3, 2):
        b = (x + d) % XS
        remote(rows_of(1 - core, b), rows_of(1 - core, b), ag_send.at[0], ag_recv.at[1 - core, b], pair).wait_recv()
    sent(o_ref.at[pl.ds(0, 3 * BLOCK), :], ag_send.at[0])
    sent(o_ref.at[pl.ds(0, 4 * BLOCK), :], ag_send.at[1])


def shards(tokens, norm_gain, qkv_weight, out_weight):
    dma = pltpu.SemaphoreType.DMA
    return pl.pallas_call(
        kernel,
        out_shape=pltpu.VMEM((T, T), BF16),
        in_specs=[
            pl.BlockSpec(memory_space=pl.ANY),
            pl.BlockSpec(memory_space=pl.ANY),
            pl.BlockSpec(memory_space=pl.ANY),
            pl.BlockSpec(memory_space=pl.ANY),
        ],
        out_specs=pl.BlockSpec(memory_space=pltpu.VMEM),
        scratch_shapes=[
            pltpu.VMEM((T, T), BF16),
            pltpu.VMEM((T,), F32),
            pltpu.VMEM((3, T, T), BF16),
            pltpu.VMEM((T, T), BF16),
            pltpu.VMEM((T + 16, T), BF16),
            pltpu.VMEM((2, 6, 8, K), F32),
            pltpu.VMEM((ZS, 2, 8, K), F32),
            pltpu.VMEM((3, 6, HALF, K), F32),
            pltpu.VMEM((2, 6, HALF, K), BF16),
            pltpu.VMEM((3, 6, HALF, K), BF16),
            pltpu.VMEM((3, 4, HALF, K), BF16),
            pltpu.VMEM((3, 3, HALF, K), BF16),
            pltpu.VMEM((3, HALF, K), F32),
            pltpu.VMEM((HALF, K), BF16),
            pltpu.VMEM((HALF, K), BF16),
            pltpu.VMEM((3, 2, HALF, K), BF16),
            pltpu.VMEM((6, HALF, K), BF16),
            pltpu.VMEM((HALF, T), BF16),
            pltpu.VMEM((HALF, T), BF16),
            pltpu.VMEM((XS, BLOCK, T), BF16),
            pltpu.VMEM((XS, BLOCK, T), BF16),
            dma((6,)),
            dma((2,)),
            dma((1,)),
            dma((1,)),
            dma((1,)),
            dma((2, 6)),
            dma((1,)),
            dma((3, 4)),
            dma((3, 3)),
            dma((2,)),
            dma((2,)),
            dma((2,)),
            dma((2,)),
            dma((6,)),
            dma((1,)),
            dma((6,)),
            dma((2,)),
            dma((2,)),
            dma((2,)),
            dma((2, XS)),
        ],
        compiler_params=pltpu.CompilerParams(collective_id=0, has_side_effects=True),
        name="sublayer",
    )(tokens, norm_gain, jnp.transpose(qkv_weight, (1, 0, 2)), out_weight)


def solution(mesh):
    in_specs = (P("dp", "row"), P("row"), P("row", None, "col"), P("col", "row"))
    out_specs = P("dp", "row")
    return jax.shard_map(shards, mesh=mesh, in_specs=in_specs, out_specs=out_specs, check_vma=False)
```

```python
import math

import jax
import jax.numpy as jnp
from jax import lax
from jax.experimental import pallas as pl
from jax.experimental.pallas import tpu as pltpu
from jax.sharding import PartitionSpec as P

K = 128
EPSILON = 1e-05
F32 = jnp.float32
BF16 = jnp.bfloat16
T = 384
HALF = 192
BLOCK = 48
ZS = 8
XS = 4
FEATURES = 6144
ORDER = (1, 2, 0)
EARLY = 2
MESH = pl.DeviceIdType.MESH


def owner_z(owner):
    return owner + owner // 3


def kernel(
    x_hbm, gain_hbm, w_hbm, wo_hbm, o_ref,
    x_v, gain_v, w_v, wo_v, lhs, aux_own, aux_all, part, y_buf, z_buf, z_in, tie_in, acc, qkv, att,
    pair_out, pair_in, p_buf, p_in,
    load_sem, aux_sems, auxz_send, auxz_recv, y_send, y_recv, z_send, z_recv, tie_recv,
    kv_send, kv_recv, at_send, at_recv, ay_send, ay_recv, pair_sems, rs_sems, ag_send, ag_recv,
):
    row = lax.axis_index("row")
    col = lax.axis_index("col")
    y = row // ZS
    z = row % ZS
    x = col // 2
    core = col % 2
    active = y == core
    partner = {"row": (1 - y) * ZS + z}
    pair = {"col": 2 * x + 1 - core}
    owns = z % 4 != 3
    is_owner = jnp.logical_and(active, owns)
    mine = z - z // 4
    head = mine // 2
    half = mine % 2

    def at_x(d):
        return {"col": 2 * ((x + d) % XS) + core}

    def at_z(other):
        return {"row": y * ZS + other}

    def remote(src, dst, send, recv, device):
        return pltpu.make_async_remote_copy(
            src_ref=src, dst_ref=dst, send_sem=send, recv_sem=recv, device_id=device, device_id_type=MESH
        )

    x_load = pltpu.make_async_copy(x_hbm, x_v, load_sem.at[0])
    x_load.start()
    w_loads = [pltpu.make_async_copy(w_hbm.at[j], w_v.at[j], load_sem.at[1 + j]) for j in range(3)]
    for j in ORDER:
        w_loads[j].start()
    gain_load = pltpu.make_async_copy(gain_hbm, gain_v, load_sem.at[5])
    gain_load.start()
    wo_load = pltpu.make_async_copy(wo_hbm, wo_v, load_sem.at[4])
    wo_load.start()

    barrier = pltpu.get_barrier_semaphore()
    pl.semaphore_signal(barrier, inc=1, device_id=partner, device_id_type=MESH)
    pl.semaphore_signal(barrier, inc=1, device_id=pair, device_id_type=MESH)
    for d in range(1, XS):
        pl.semaphore_signal(barrier, inc=1, device_id=at_x(d), device_id_type=MESH)
    @pl.when(active)
    def _():
        pl.semaphore_signal(barrier, inc=1, device_id=at_z((z + 7) % ZS), device_id_type=MESH)

    @pl.when(is_owner)
    def _():
        for d in range(1, ZS - 1):
            pl.semaphore_signal(barrier, inc=1, device_id=at_z((z + d) % ZS), device_id_type=MESH)

    arrivals = 5 + jnp.where(active, jnp.where(owns, 5, 6) + jnp.where(z % 4 == 2, 1, 0), 0)

    x_load.wait()
    values = x_v[...].astype(F32)
    mean = jnp.sum(values, axis=1, keepdims=True) * (1.0 / T)
    centered = values - mean
    squares = jnp.sum(centered * centered, axis=1, keepdims=True)
    gain_load.wait()
    gain = gain_v[...].reshape(1, T)
    lhs[0:T, :] = (centered * gain).astype(BF16)
    high = gain.astype(BF16).astype(F32)
    rows = lax.broadcasted_iota(jnp.int32, (16, T), 0)
    lhs[T : T + 16, :] = jnp.where(rows == 0, high, jnp.where(rows == 1, gain - high, 0.0)).astype(BF16)
    lanes = lax.broadcasted_iota(jnp.int32, (T, 128), 1)
    turned = jnp.where(lanes == 0, mean, jnp.where(lanes == 1, squares, 0.0)).T
    early = turned[0:8, :]
    late = pltpu.roll(early, T - HALF, 1)
    for o in range(6):
        source = early if o % 2 == 0 else late
        for r in range(2):
            aux_own[0, o, 3 + 2 * r : 4 + 2 * r, :] = source[r : r + 1, 0:K]
            aux_own[0, o, 4 + 2 * r : 5 + 2 * r, :] = source[r : r + 1, K : 2 * K]

    tie = (z + 4) % ZS
    first = jnp.where(tie % 4 == 3, (tie + 1) % ZS, tie)
    first = first - first // 4

    def order(i):
        return (first + i) % 6

    def y_copy(n, o):
        return remote(y_buf.at[n, o], y_buf.at[n, o], y_send.at[0], y_recv.at[n, o], partner)

    aux_copy = remote(aux_own.at[0], aux_own.at[1], aux_sems.at[0], aux_sems.at[1], partner)

    def z_copy(j, o, to):
        return remote(z_buf.at[j, o], z_in.at[z, j], z_send.at[0], z_recv.at[j], at_z(to))

    def tie_copy(j, o):
        return remote(z_buf.at[j, o], tie_in.at[j], z_send.at[0], tie_recv.at[j], at_z((z + 1) % ZS))

    def aux_z_copy(o):
        return remote(aux_own.at[:, o], aux_all.at[z], auxz_send.at[0], auxz_recv.at[0], at_z(owner_z(o)))

    for step, j in enumerate(ORDER):
        w_loads[j].wait()
        product = jnp.dot(lhs[...], w_v[j], preferred_element_type=F32)
        weights_sum = product[T : T + 1, :] + product[T + 1 : T + 2, :]
        for o in range(6):
            aux_own[0, o, j : j + 1, :] = weights_sum[:, (o // 2) * K : (o // 2 + 1) * K]

        def piece(o):
            return product[(o % 2) * HALF : (o % 2 + 1) * HALF, (o // 2) * K : (o // 2 + 1) * K]

        @pl.when(active)
        def _():
            for o in range(6):
                part[j, o] = piece(o)

        @pl.when(jnp.logical_not(active))
        def _():
            for o in range(6):
                y_buf[j, o] = piece(o).astype(BF16)

        if step == 0:
            pl.semaphore_wait(barrier, arrivals)

        @pl.when(jnp.logical_not(active))
        def _(step=step):
            if step == 0:
                for i in range(EARLY):
                    y_copy(ORDER[0], order(i)).start()
            if step == 2:
                aux_copy.start()
                for i in range(EARLY, 18):
                    y_copy(ORDER[i // 6], order(i % 6)).start()

    @pl.when(active)
    def _():
        for i in range(18):
            j = ORDER[i // 6]
            o = order(i % 6)
            to = owner_z(o)
            ahead = (to - z + ZS) % ZS

            if i == EARLY:
                aux_copy.wait_recv()
                for owner in range(6):
                    @pl.when(z != owner_z(owner))
                    def _(owner=owner):
                        aux_z_copy(owner).start()

                    @pl.when(z == owner_z(owner))
                    def _(owner=owner):
                        aux_all[z] = aux_own[:, owner]

            y_copy(j, o).wait_recv()
            total = part[j, o] + y_buf[j, o].astype(F32)

            @pl.when(ahead == 0)
            def _(j=j, total=total):
                acc[j] = total

            @pl.when(ahead == 4)
            def _(j=j, o=o, total=total):
                z_buf[j, o] = total.astype(BF16)
                tie_copy(j, o).start()

            @pl.when(ahead == 3)
            def _(i=i, j=j, o=o, to=to, total=total):
                tie_copy(j, o).wait_recv()
                z_buf[j, o] = (total + tie_in[j].astype(F32)).astype(BF16)
                z_copy(j, o, to).start()

            @pl.when(jnp.logical_and(ahead != 0, jnp.logical_and(ahead != 3, ahead != 4)))
            def _(j=j, o=o, to=to, total=total):
                z_buf[j, o] = total.astype(BF16)
                z_copy(j, o, to).start()

    def kv_copy(j):
        return remote(
            qkv.at[j, half], qkv.at[j, half], kv_send.at[j - 1], kv_recv.at[j - 1], at_z(owner_z(mine + 1 - 2 * half))
        )

    def at_copy(d):
        return remote(att.at[mine], att.at[mine], at_send.at[0], at_recv.at[mine], at_z((z + d) % ZS))

    def at_forward(o):
        return remote(att.at[o], att.at[o], at_send.at[1], at_recv.at[o], at_z((z + 1) % ZS))

    def ay_copy(o):
        return remote(att.at[o], att.at[o], ay_send.at[0], ay_recv.at[o], partner)

    def summed(j, start):
        remote(z_in.at[pl.ds(0, 6), 0], z_in.at[pl.ds(0, 6), j], z_send.at[0], z_recv.at[j], partner).wait_recv()
        total = start
        for d in (1, 7, 2, 6, 5, 3):
            total = total + z_in[(z + ZS - d) % ZS, j].astype(F32)
        return total

    @pl.when(is_owner)
    def _():
        remote(
            aux_all.at[pl.ds(0, 7)], aux_all.at[pl.ds(0, 7)], auxz_send.at[0], auxz_recv.at[0], partner
        ).wait_recv()

        def gathered(r):
            return aux_all[:, :, r, :].reshape(2 * ZS, K)

        means = jnp.concatenate([gathered(3), gathered(4)], axis=1)
        average = jnp.sum(means, axis=0, keepdims=True) * (1.0 / 16)
        offsets = means - average
        sums = jnp.concatenate([gathered(5), gathered(6)], axis=1)
        spread = jnp.sum(sums + T * (offsets * offsets), axis=0, keepdims=True) * (1.0 / FEATURES)
        scale = lax.rsqrt(spread + EPSILON)
        tall = jnp.concatenate([offsets, jnp.broadcast_to(scale, (112, 2 * K))], axis=0).T
        scale_col = tall[0:HALF, 16:17]
        offset_cols = tall[0:HALF, 0:16]

        for j in ORDER:
            start = acc[j] + jnp.dot(
                offset_cols, gathered(j), preferred_element_type=F32, precision=lax.Precision.HIGHEST
            )
            qkv[j, half] = (summed(j, start) * scale_col).astype(BF16)
            if j > 0:
                kv_copy(j).start()

        kv_copy(1).wait_recv()
        queries = qkv[0, half]
        keys = qkv[1].reshape(T, K)
        scores = lax.dot_general(
            queries, keys, (((1,), (1,)), ((), ())), preferred_element_type=F32
        ) * (1.0 / math.sqrt(K))
        exponent = jnp.exp(scores - jnp.max(scores, axis=1, keepdims=True))
        weights = (exponent / jnp.sum(exponent, axis=1, keepdims=True)).astype(BF16)
        kv_copy(2).wait_recv()
        mixed = jnp.dot(weights, qkv[2].reshape(T, K), preferred_element_type=F32)
        att[mine] = mixed.astype(BF16)
        for d in (3, 5, 2, 6, 1, 7):
            at_copy(d).start()

    pair_copy = remote(pair_out, pair_in, pair_sems.at[0], pair_sems.at[1], pair)

    def rs_copy(d):
        return remote(p_buf.at[(x + d) % XS], p_in.at[x], rs_sems.at[0], rs_sems.at[1], at_x(d))

    for n in range(2):
        s = jnp.where(n == 0, 1 - core, core)

        @pl.when(active)
        def _(s=s, n=n):
            for h in range(3):
                o = 2 * h + s

                @pl.when(z != owner_z(o))
                def _(o=o, h=h):
                    remote(att.at[o], att.at[o], at_send.at[0], at_recv.at[o], partner).wait_recv()

                @pl.when(z == (owner_z(o) + 3) % ZS)
                def _(o=o):
                    at_forward(o).start()

                ay_copy(o).start()

        @pl.when(jnp.logical_not(active))
        def _(s=s, n=n):
            for h in range(3):
                ay_copy(2 * h + s).wait_recv()

        if n == 0:
            wo_load.wait()
        attended = jnp.concatenate([att[2 * h + s] for h in range(3)], axis=1)
        product = jnp.dot(attended, wo_v[...], preferred_element_type=F32)
        if n == 0:
            pair_out[...] = product.astype(BF16)
            pair_copy.start()
        else:
            pair_copy.wait_recv()
            both = (product + pair_in[...].astype(F32)).astype(BF16)
            for b in range(XS):
                p_buf[b] = both[b * BLOCK : (b + 1) * BLOCK, :]
            for d in (2, 1, 3):
                rs_copy(d).start()

    def rows_of(k, b):
        return o_ref.at[pl.ds(pl.multiple_of(k * HALF + b * BLOCK, BLOCK), BLOCK), :]

    def ag_copy(b, n, device):
        rows = rows_of(core, b)
        return remote(rows, rows, ag_send.at[n], ag_recv.at[core, b], device)

    remote(p_in.at[pl.ds(0, 3)], p_in.at[pl.ds(0, 3)], rs_sems.at[0], rs_sems.at[1], pair).wait_recv()
    total = p_buf[x].astype(F32)
    for d in (1, 3, 2):
        total = total + p_in[(x + d) % XS].astype(F32)
    rows_of(core, x)[...] = total.astype(BF16)
    for d in (2, 1, 3):
        ag_copy(x, 0, at_x(d)).start()
    ag_copy(x, 1, pair).start()

    def sent(ref, sem):
        remote(ref, ref, sem, sem, pair).wait_send()

    @pl.when(jnp.logical_not(active))
    def _():
        aux_copy.wait_send()
        sent(y_buf, y_send.at[0])

    @pl.when(active)
    def _():
        sent(att, ay_send.at[0])

        @pl.when(z % 4 != 2)
        def _():
            sent(att.at[0], at_send.at[1])

        @pl.when(owns)
        def _():
            sent(aux_all.at[pl.ds(0, 5)], auxz_send.at[0])
            sent(z_buf.at[:, pl.ds(0, 5)], z_send.at[0])
            kv_copy(1).wait_send()
            kv_copy(2).wait_send()
            sent(att, at_send.at[0])

        @pl.when(jnp.logical_not(owns))
        def _():
            sent(aux_all.at[pl.ds(0, 6)], auxz_send.at[0])
            sent(z_buf, z_send.at[0])

    pair_copy.wait_send()
    sent(p_in.at[pl.ds(0, 3)], rs_sems.at[0])

    for d in (1, 3, 2):
        b = (x + d) % XS
        ag_copy(b, 0, pair).wait_recv()
        ag_copy(b, 1, pair).start()
    for d in (0, 1, 3, 2):
        b = (x + d) % XS
        remote(rows_of(1 - core, b), rows_of(1 - core, b), ag_send.at[0], ag_recv.at[1 - core, b], pair).wait_recv()
    sent(o_ref.at[pl.ds(0, 3 * BLOCK), :], ag_send.at[0])
    sent(o_ref.at[pl.ds(0, 4 * BLOCK), :], ag_send.at[1])


def shards(tokens, norm_gain, qkv_weight, out_weight):
    dma = pltpu.SemaphoreType.DMA
    return pl.pallas_call(
        kernel,
        out_shape=pltpu.VMEM((T, T), BF16),
        in_specs=[
            pl.BlockSpec(memory_space=pl.ANY),
            pl.BlockSpec(memory_space=pl.ANY),
            pl.BlockSpec(memory_space=pl.ANY),
            pl.BlockSpec(memory_space=pl.ANY),
        ],
        out_specs=pl.BlockSpec(memory_space=pltpu.VMEM),
        scratch_shapes=[
            pltpu.VMEM((T, T), BF16),
            pltpu.VMEM((T,), F32),
            pltpu.VMEM((3, T, T), BF16),
            pltpu.VMEM((T, T), BF16),
            pltpu.VMEM((T + 16, T), BF16),
            pltpu.VMEM((2, 6, 8, K), F32),
            pltpu.VMEM((ZS, 2, 8, K), F32),
            pltpu.VMEM((3, 6, HALF, K), F32),
            pltpu.VMEM((3, 6, HALF, K), BF16),
            pltpu.VMEM((3, 6, HALF, K), BF16),
            pltpu.VMEM((ZS, 3, HALF, K), BF16),
            pltpu.VMEM((3, HALF, K), BF16),
            pltpu.VMEM((3, HALF, K), F32),
            pltpu.VMEM((3, 2, HALF, K), BF16),
            pltpu.VMEM((6, HALF, K), BF16),
            pltpu.VMEM((HALF, T), BF16),
            pltpu.VMEM((HALF, T), BF16),
            pltpu.VMEM((XS, BLOCK, T), BF16),
            pltpu.VMEM((XS, BLOCK, T), BF16),
            dma((6,)),
            dma((2,)),
            dma((1,)),
            dma((1,)),
            dma((1,)),
            dma((3, 6)),
            dma((1,)),
            dma((3,)),
            dma((3,)),
            dma((2,)),
            dma((2,)),
            dma((2,)),
            dma((6,)),
            dma((1,)),
            dma((6,)),
            dma((2,)),
            dma((2,)),
            dma((2,)),
            dma((2, XS)),
        ],
        compiler_params=pltpu.CompilerParams(collective_id=0, has_side_effects=True),
        name="sublayer",
    )(tokens, norm_gain, jnp.transpose(qkv_weight, (1, 0, 2)), out_weight)


def solution(mesh):
    in_specs = (P("dp", "row"), P("row"), P("row", None, "col"), P("col", "row"))
    out_specs = P("dp", "row")
    return jax.shard_map(shards, mesh=mesh, in_specs=in_specs, out_specs=out_specs, check_vma=False)
```

```python
import math

import jax
import jax.numpy as jnp
from jax import lax
from jax.experimental import pallas as pl
from jax.experimental.pallas import tpu as pltpu
from jax.sharding import PartitionSpec as P

K = 128
EPSILON = 1e-05
F32 = jnp.float32
BF16 = jnp.bfloat16
T = 384
HALF = 192
BLOCK = 48
ZS = 8
XS = 4
FEATURES = 6144
ORDER = (1, 2, 0)
EARLY = 2
NEAREST = ((0, 1, 2, 6, 5, 4), (0, 1, 7, 3, 5, 4), (0, 7, 2, 6, 3, 4), (1, 7, 2, 6, 3, 5))
MESH = pl.DeviceIdType.MESH


def owner_z(owner):
    return owner + owner // 3


def kernel(
    x_hbm, gain_hbm, w_hbm, wo_hbm, o_ref,
    x_v, gain_v, w_v, wo_v, lhs, aux_own, aux_all, part, y_buf, z_buf, z_in, tie_in, acc, qkv, att,
    out_acc, pair_out, pair_in, p_buf, p_in,
    load_sem, aux_sems, auxz_send, auxz_recv, y_send, y_recv, z_send, z_recv, tie_recv,
    kv_send, kv_recv, at_send, at_recv, ay_send, ay_recv, pair_sems, rs_sems, ag_send, ag_recv,
):
    row = lax.axis_index("row")
    col = lax.axis_index("col")
    y = row // ZS
    z = row % ZS
    x = col // 2
    core = col % 2
    active = y == core
    partner = {"row": (1 - y) * ZS + z}
    pair = {"col": 2 * x + 1 - core}
    owns = z % 4 != 3
    is_owner = jnp.logical_and(active, owns)
    mine = z - z // 4
    head = mine // 2
    half = mine % 2

    def at_x(d):
        return {"col": 2 * ((x + d) % XS) + core}

    def at_z(other):
        return {"row": y * ZS + other}

    def remote(src, dst, send, recv, device):
        return pltpu.make_async_remote_copy(
            src_ref=src, dst_ref=dst, send_sem=send, recv_sem=recv, device_id=device, device_id_type=MESH
        )

    x_load = pltpu.make_async_copy(x_hbm, x_v, load_sem.at[0])
    x_load.start()
    w_loads = [pltpu.make_async_copy(w_hbm.at[j], w_v.at[j], load_sem.at[1 + j]) for j in range(3)]
    for j in ORDER:
        w_loads[j].start()
    gain_load = pltpu.make_async_copy(gain_hbm, gain_v, load_sem.at[5])
    gain_load.start()
    wo_load = pltpu.make_async_copy(wo_hbm, wo_v, load_sem.at[4])
    wo_load.start()

    barrier = pltpu.get_barrier_semaphore()
    pl.semaphore_signal(barrier, inc=1, device_id=partner, device_id_type=MESH)
    pl.semaphore_signal(barrier, inc=1, device_id=pair, device_id_type=MESH)
    for d in range(1, XS):
        pl.semaphore_signal(barrier, inc=1, device_id=at_x(d), device_id_type=MESH)
    @pl.when(active)
    def _():
        pl.semaphore_signal(barrier, inc=1, device_id=at_z((z + 7) % ZS), device_id_type=MESH)

    @pl.when(is_owner)
    def _():
        for d in range(1, ZS - 1):
            pl.semaphore_signal(barrier, inc=1, device_id=at_z((z + d) % ZS), device_id_type=MESH)

    arrivals = 5 + jnp.where(active, jnp.where(owns, 5, 6) + jnp.where(z % 4 == 2, 1, 0), 0)

    x_load.wait()
    values = x_v[...].astype(F32)
    mean = jnp.sum(values, axis=1, keepdims=True) * (1.0 / T)
    centered = values - mean
    squares = jnp.sum(centered * centered, axis=1, keepdims=True)
    gain_load.wait()
    gain = gain_v[...].reshape(1, T)
    lhs[0:T, :] = (centered * gain).astype(BF16)
    high = gain.astype(BF16).astype(F32)
    rows = lax.broadcasted_iota(jnp.int32, (16, T), 0)
    lhs[T : T + 16, :] = jnp.where(rows == 0, high, jnp.where(rows == 1, gain - high, 0.0)).astype(BF16)
    lanes = lax.broadcasted_iota(jnp.int32, (T, 128), 1)
    turned = jnp.where(lanes == 0, mean, jnp.where(lanes == 1, squares, 0.0)).T
    early = turned[0:8, :]
    late = pltpu.roll(early, T - HALF, 1)
    for o in range(6):
        source = early if o % 2 == 0 else late
        for r in range(2):
            aux_own[0, o, 3 + 2 * r : 4 + 2 * r, :] = source[r : r + 1, 0:K]
            aux_own[0, o, 4 + 2 * r : 5 + 2 * r, :] = source[r : r + 1, K : 2 * K]

    tie = (z + 4) % ZS
    first = jnp.where(tie % 4 == 3, (tie + 1) % ZS, tie)
    first = first - first // 4

    def order(i):
        return (first + i) % 6

    def y_copy(n, o):
        return remote(y_buf.at[n, o], y_buf.at[n, o], y_send.at[0], y_recv.at[n, o], partner)

    aux_copy = remote(aux_own.at[0], aux_own.at[1], aux_sems.at[0], aux_sems.at[1], partner)

    def z_copy(j, o, to):
        return remote(z_buf.at[j, o], z_in.at[z, j], z_send.at[0], z_recv.at[j], at_z(to))

    def tie_copy(j, o):
        return remote(z_buf.at[j, o], tie_in.at[j], z_send.at[0], tie_recv.at[j], at_z((z + 1) % ZS))

    def aux_z_copy(o):
        return remote(aux_own.at[:, o], aux_all.at[z], auxz_send.at[0], auxz_recv.at[0], at_z(owner_z(o)))

    for step, j in enumerate(ORDER):
        w_loads[j].wait()
        product = jnp.dot(lhs[...], w_v[j], preferred_element_type=F32)
        weights_sum = product[T : T + 1, :] + product[T + 1 : T + 2, :]
        for o in range(6):
            aux_own[0, o, j : j + 1, :] = weights_sum[:, (o // 2) * K : (o // 2 + 1) * K]

        def piece(o):
            return product[(o % 2) * HALF : (o % 2 + 1) * HALF, (o // 2) * K : (o // 2 + 1) * K]

        @pl.when(active)
        def _():
            for o in range(6):
                part[j, o] = piece(o)

        @pl.when(jnp.logical_not(active))
        def _():
            for o in range(6):
                y_buf[j, o] = piece(o).astype(BF16)

        if step == 0:
            pl.semaphore_wait(barrier, arrivals)

        @pl.when(jnp.logical_not(active))
        def _(step=step):
            if step == 0:
                for i in range(EARLY):
                    y_copy(ORDER[0], order(i)).start()
            if step == 2:
                aux_copy.start()
                for i in range(EARLY, 18):
                    y_copy(ORDER[i // 6], order(i % 6)).start()

    @pl.when(active)
    def _():
        for i in range(18):
            j = ORDER[i // 6]
            o = order(i % 6)
            to = owner_z(o)
            ahead = (to - z + ZS) % ZS

            if i == EARLY:
                aux_copy.wait_recv()
                for owner in range(6):
                    @pl.when(z != owner_z(owner))
                    def _(owner=owner):
                        aux_z_copy(owner).start()

                    @pl.when(z == owner_z(owner))
                    def _(owner=owner):
                        aux_all[z] = aux_own[:, owner]

            y_copy(j, o).wait_recv()
            total = part[j, o] + y_buf[j, o].astype(F32)

            @pl.when(ahead == 0)
            def _(j=j, total=total):
                acc[j] = total

            @pl.when(ahead == 4)
            def _(j=j, o=o, total=total):
                z_buf[j, o] = total.astype(BF16)
                tie_copy(j, o).start()

            @pl.when(ahead == 3)
            def _(i=i, j=j, o=o, to=to, total=total):
                tie_copy(j, o).wait_recv()
                z_buf[j, o] = (total + tie_in[j].astype(F32)).astype(BF16)
                z_copy(j, o, to).start()

            @pl.when(jnp.logical_and(ahead != 0, jnp.logical_and(ahead != 3, ahead != 4)))
            def _(j=j, o=o, to=to, total=total):
                z_buf[j, o] = total.astype(BF16)
                z_copy(j, o, to).start()

    def kv_copy(j):
        return remote(
            qkv.at[j, half], qkv.at[j, half], kv_send.at[j - 1], kv_recv.at[j - 1], at_z(owner_z(mine + 1 - 2 * half))
        )

    def at_copy(d):
        return remote(att.at[mine], att.at[mine], at_send.at[int(d == 4)], at_recv.at[mine], at_z((z + d) % ZS))

    def ay_copy(o):
        return remote(att.at[o], att.at[o], ay_send.at[0], ay_recv.at[o], partner)

    def summed(j, start):
        remote(z_in.at[pl.ds(0, 6), 0], z_in.at[pl.ds(0, 6), j], z_send.at[0], z_recv.at[j], partner).wait_recv()
        total = start
        for d in (1, 7, 2, 6, 5, 3):
            total = total + z_in[(z + ZS - d) % ZS, j].astype(F32)
        return total

    @pl.when(is_owner)
    def _():
        remote(
            aux_all.at[pl.ds(0, 7)], aux_all.at[pl.ds(0, 7)], auxz_send.at[0], auxz_recv.at[0], partner
        ).wait_recv()

        def gathered(r):
            return aux_all[:, :, r, :].reshape(2 * ZS, K)

        means = jnp.concatenate([gathered(3), gathered(4)], axis=1)
        average = jnp.sum(means, axis=0, keepdims=True) * (1.0 / 16)
        offsets = means - average
        sums = jnp.concatenate([gathered(5), gathered(6)], axis=1)
        spread = jnp.sum(sums + T * (offsets * offsets), axis=0, keepdims=True) * (1.0 / FEATURES)
        scale = lax.rsqrt(spread + EPSILON)
        tall = jnp.concatenate([offsets, jnp.broadcast_to(scale, (112, 2 * K))], axis=0).T
        scale_col = tall[0:HALF, 16:17]
        offset_cols = tall[0:HALF, 0:16]

        for j in ORDER:
            start = acc[j] + jnp.dot(
                offset_cols, gathered(j), preferred_element_type=F32, precision=lax.Precision.HIGHEST
            )
            qkv[j, half] = (summed(j, start) * scale_col).astype(BF16)
            if j > 0:
                kv_copy(j).start()

        kv_copy(1).wait_recv()
        queries = qkv[0, half]
        keys = qkv[1].reshape(T, K)
        scores = lax.dot_general(
            queries, keys, (((1,), (1,)), ((), ())), preferred_element_type=F32
        ) * (1.0 / math.sqrt(K))
        exponent = jnp.exp(scores - jnp.max(scores, axis=1, keepdims=True))
        weights = (exponent / jnp.sum(exponent, axis=1, keepdims=True)).astype(BF16)
        kv_copy(2).wait_recv()
        mixed = jnp.dot(weights, qkv[2].reshape(T, K), preferred_element_type=F32)
        att[mine] = mixed.astype(BF16)
        for d in (4, 3, 5, 2, 6, 1, 7):
            at_copy(d).start()

    pair_copy = remote(pair_out, pair_in, pair_sems.at[0], pair_sems.at[1], pair)

    def rs_copy(d):
        return remote(p_buf.at[(x + d) % XS], p_in.at[x], rs_sems.at[0], rs_sems.at[1], at_x(d))

    out_acc[...] = jnp.zeros_like(out_acc)
    wo_load.wait()
    kind = z % 4
    for i in range(6):
        near = [table[i] for table in NEAREST]
        there = jnp.where(kind == 0, near[0], jnp.where(kind == 1, near[1], jnp.where(kind == 2, near[2], near[3])))
        source = (z + there) % ZS
        o = source - source // 4

        @pl.when(active)
        def _(o=o, i=i, there=there):
            @pl.when(there != 0)
            def _():
                remote(att.at[o], att.at[o], at_send.at[0], at_recv.at[o], partner).wait_recv()

            ay_copy(o).start()

        @pl.when(jnp.logical_not(active))
        def _(o=o, i=i):
            ay_copy(o).wait_recv()

        weights = wo_v[pl.ds(pl.multiple_of((o // 2) * K, K), K), :]
        out_acc[o % 2] += jnp.dot(att[o], weights, preferred_element_type=F32)

    pair_out[...] = out_acc[1 - core].astype(BF16)
    pair_copy.start()
    mine_f32 = out_acc[core]
    pair_copy.wait_recv()
    both = (mine_f32 + pair_in[...].astype(F32)).astype(BF16)
    for b in range(XS):
        p_buf[b] = both[b * BLOCK : (b + 1) * BLOCK, :]
    for d in (2, 1, 3):
        rs_copy(d).start()

    def rows_of(k, b):
        return o_ref.at[pl.ds(pl.multiple_of(k * HALF + b * BLOCK, BLOCK), BLOCK), :]

    def ag_copy(b, n, device):
        rows = rows_of(core, b)
        return remote(rows, rows, ag_send.at[n], ag_recv.at[core, b], device)

    remote(p_in.at[pl.ds(0, 3)], p_in.at[pl.ds(0, 3)], rs_sems.at[0], rs_sems.at[1], pair).wait_recv()
    total = p_buf[x].astype(F32)
    for d in (1, 3, 2):
        total = total + p_in[(x + d) % XS].astype(F32)
    rows_of(core, x)[...] = total.astype(BF16)
    for d in (2, 1, 3):
        ag_copy(x, 0, at_x(d)).start()
    ag_copy(x, 1, pair).start()

    def sent(ref, sem):
        remote(ref, ref, sem, sem, pair).wait_send()

    @pl.when(jnp.logical_not(active))
    def _():
        aux_copy.wait_send()
        sent(y_buf, y_send.at[0])

    @pl.when(active)
    def _():
        sent(att, ay_send.at[0])

        @pl.when(owns)
        def _():
            sent(aux_all.at[pl.ds(0, 5)], auxz_send.at[0])
            sent(z_buf.at[:, pl.ds(0, 5)], z_send.at[0])
            kv_copy(1).wait_send()
            kv_copy(2).wait_send()
            sent(att, at_send.at[0])
            sent(att.at[0], at_send.at[1])

        @pl.when(jnp.logical_not(owns))
        def _():
            sent(aux_all.at[pl.ds(0, 6)], auxz_send.at[0])
            sent(z_buf, z_send.at[0])

    pair_copy.wait_send()
    sent(p_in.at[pl.ds(0, 3)], rs_sems.at[0])

    for d in (1, 3, 2):
        b = (x + d) % XS
        ag_copy(b, 0, pair).wait_recv()
        ag_copy(b, 1, pair).start()
    for d in (0, 1, 3, 2):
        b = (x + d) % XS
        remote(rows_of(1 - core, b), rows_of(1 - core, b), ag_send.at[0], ag_recv.at[1 - core, b], pair).wait_recv()
    sent(o_ref.at[pl.ds(0, 3 * BLOCK), :], ag_send.at[0])
    sent(o_ref.at[pl.ds(0, 4 * BLOCK), :], ag_send.at[1])


def shards(tokens, norm_gain, qkv_weight, out_weight):
    dma = pltpu.SemaphoreType.DMA
    return pl.pallas_call(
        kernel,
        out_shape=pltpu.VMEM((T, T), BF16),
        in_specs=[
            pl.BlockSpec(memory_space=pl.ANY),
            pl.BlockSpec(memory_space=pl.ANY),
            pl.BlockSpec(memory_space=pl.ANY),
            pl.BlockSpec(memory_space=pl.ANY),
        ],
        out_specs=pl.BlockSpec(memory_space=pltpu.VMEM),
        scratch_shapes=[
            pltpu.VMEM((T, T), BF16),
            pltpu.VMEM((T,), F32),
            pltpu.VMEM((3, T, T), BF16),
            pltpu.VMEM((T, T), BF16),
            pltpu.VMEM((T + 16, T), BF16),
            pltpu.VMEM((2, 6, 8, K), F32),
            pltpu.VMEM((ZS, 2, 8, K), F32),
            pltpu.VMEM((3, 6, HALF, K), F32),
            pltpu.VMEM((3, 6, HALF, K), BF16),
            pltpu.VMEM((3, 6, HALF, K), BF16),
            pltpu.VMEM((ZS, 3, HALF, K), BF16),
            pltpu.VMEM((3, HALF, K), BF16),
            pltpu.VMEM((3, HALF, K), F32),
            pltpu.VMEM((3, 2, HALF, K), BF16),
            pltpu.VMEM((6, HALF, K), BF16),
            pltpu.VMEM((2, HALF, T), F32),
            pltpu.VMEM((HALF, T), BF16),
            pltpu.VMEM((HALF, T), BF16),
            pltpu.VMEM((XS, BLOCK, T), BF16),
            pltpu.VMEM((XS, BLOCK, T), BF16),
            dma((6,)),
            dma((2,)),
            dma((1,)),
            dma((1,)),
            dma((1,)),
            dma((3, 6)),
            dma((1,)),
            dma((3,)),
            dma((3,)),
            dma((2,)),
            dma((2,)),
            dma((2,)),
            dma((6,)),
            dma((1,)),
            dma((6,)),
            dma((2,)),
            dma((2,)),
            dma((2,)),
            dma((2, XS)),
        ],
        compiler_params=pltpu.CompilerParams(collective_id=0, has_side_effects=True),
        name="sublayer",
    )(tokens, norm_gain, jnp.transpose(qkv_weight, (1, 0, 2)), out_weight)


def solution(mesh):
    in_specs = (P("dp", "row"), P("row"), P("row", None, "col"), P("col", "row"))
    out_specs = P("dp", "row")
    return jax.shard_map(shards, mesh=mesh, in_specs=in_specs, out_specs=out_specs, check_vma=False)
```
